512 devices in a mesh: trans: 64 (over z, x, y_hi), los: 8 (over y_lo, core).
Axes of the slice: x: 4, y: 8 (y_hi: 2, y_lo: 4; y = y_hi * 4 + y_lo), z: 8, core: 2. Of those that a mesh axis runs over, the one named last changes fastest.
Arguments:
- density: bfloat16 [8, 2048, 2048], P('los', 'trans'), may hold values from -6 to 6
- row_pos: float32 [8, 2048], replicated, may hold values from 0 to 2048
- col_pos: float32 [8, 2048], replicated, may hold values from 0 to 2048
- plane_of_slot: int32 [8], replicated, may hold values from 0 to 7, each once
- plane_bin: int32 [8], replicated, may hold values from 0 to 3, as said below
- efficiency: float32 [4, 8], replicated, may hold values from 0.3 to 3
Outputs:
- shear: float32 [2, 4, 2048, 2048], P(None, None, ('trans', 'los'))
The draws below stay inside these ranges and needn't reach their ends.
Inputs may be any that keep to these rules, and one draw needn't show every extreme that they name: `plane_bin`: some plane has bin 0 and some plane has bin 4 - 1.
All inputs are finite; a program needn't handle non-finite values.
Results may differ from the reference program's by a relative error of at most 0.006.
Values may be sent and summed in bfloat16 or wider, within the bound.
No kernel may reach another device: no remote copies, remote signals or barrier semaphores. Data moves between devices by JAX's collectives and lax.ppermute only.
A program may use at most 64 MiB of HBM per device.

```python
import math
import jax
import jax.numpy as jnp
from jax import lax

GRID = 2048
MESH = 2048
BINS = 4
PLANES = 8


def positions_for(key, salt):
    scale_key = jax.random.fold_in(key, salt)
    offset_key = jax.random.fold_in(key, salt + 1)
    lower = 0.8
    scale = jax.random.uniform(scale_key, (PLANES, 1), jnp.float32, lower, 1.0)
    offset = jax.random.uniform(offset_key, (PLANES, 1), jnp.float32, 0.0, 1.0 * MESH)
    cells = jnp.arange(GRID, dtype=jnp.int32).astype(jnp.float32)
    return jnp.mod(offset + scale * cells[None, :], 1.0 * MESH).astype(jnp.float32)


def draw_row_pos(key, part):
    return positions_for(key, 31)


def draw_col_pos(key, part):
    return positions_for(key, 41)


def draw_plane_bin(key, part):
    first_key = jax.random.fold_in(key, 11)
    second_key = jax.random.fold_in(key, 12)
    drawn = jax.random.randint(first_key, (PLANES,), 0, BINS)
    forced = jax.random.randint(second_key, (), 0, PLANES)
    other = (forced + 1) % PLANES
    plane_index = jnp.arange(PLANES, dtype=jnp.int32)
    result = jnp.where(plane_index == forced, 0, drawn)
    result = jnp.where(plane_index == other, BINS - 1, result)
    return result.astype(jnp.int32)


def steps_of(own_key, extent, cuts, smallest, high):
    loudness, own = 1.0, jax.random.fold_in(own_key, 6)
    for dim, blocks in cuts:
        steps = jnp.exp(jax.random.uniform(jax.random.fold_in(own, dim), (blocks,), jnp.float32, smallest / len(cuts), high / len(cuts)))
        loudness = loudness * jnp.repeat(steps, extent[dim] // blocks).reshape([-1 if axis == dim else 1 for axis in range(len(extent))])
    return loudness


def noise(key, extent, width, limit, shards=(), held_as=jnp.bfloat16):
    level = steps_of(key, extent, shards, -0.22, 0.18) if shards else 1.0
    entries = jax.random.normal(key, extent, jnp.float32) * width * level
    return jnp.minimum(jnp.maximum(entries, -limit), limit).astype(held_as)


def setup_inputs(seed: int = 0) -> dict:
    streams_of = jax.random.split(jax.random.key(seed), 7)
    return {
        "density": noise(streams_of[0], (PLANES, MESH, MESH), 1.0, 6.0, ((0, 8), (1, 64))),
        "row_pos": draw_row_pos(jax.random.fold_in(streams_of[6], 71), 0),
        "col_pos": draw_col_pos(jax.random.fold_in(streams_of[6], 71), 0),
        "plane_of_slot": jax.random.permutation(streams_of[3], PLANES).astype(jnp.int32),
        "plane_bin": draw_plane_bin(jax.random.fold_in(streams_of[6], 71), 0),
        "efficiency": jnp.clip(jnp.exp(jax.random.uniform(streams_of[5], (BINS, PLANES), jnp.float32, math.log(0.3), math.log(3.0))), 0.3, 3.0),
    }


def hat_block(positions, mesh_cells):
    cells = jnp.arange(mesh_cells, dtype=jnp.int32).astype(jnp.float32)
    offset = positions[:, None] - cells[None, :] + 0.5 * mesh_cells
    folded = jnp.mod(offset, 1.0 * mesh_cells) - 0.5 * mesh_cells
    return jnp.maximum(1.0 - jnp.abs(folded), 0.0).astype(jnp.bfloat16)


def wave_numbers(length):
    index_all = jnp.arange(length, dtype=jnp.int32)
    return jnp.where(index_all < length // 2, index_all, index_all - length).astype(jnp.float32)


def shear_factors(wave_rows, wave_cols):
    square_sum = jnp.maximum(wave_rows * wave_rows + wave_cols * wave_cols, 1.0)
    return (wave_rows * wave_rows - wave_cols * wave_cols) / square_sum, 2.0 * wave_rows * wave_cols / square_sum


def reference(density, row_pos, col_pos, plane_of_slot, plane_bin, efficiency):
    planes_total = density.shape[0]
    mesh_cells = density.shape[2]
    bins_total = efficiency.shape[0]
    grid_cells = row_pos.shape[1]
    convergence = jnp.zeros((bins_total, grid_cells, grid_cells), jnp.float32)
    for slot_index in range(planes_total):
        plane_id = plane_of_slot[slot_index]
        row_weights = hat_block(row_pos[plane_id], mesh_cells)
        col_weights = hat_block(col_pos[plane_id], mesh_cells)
        half_product = jnp.dot(row_weights, density[slot_index], preferred_element_type=jnp.float32).astype(jnp.bfloat16)
        plane_map = jnp.dot(half_product, col_weights.T, preferred_element_type=jnp.float32)
        weights = efficiency[:, plane_id] * (jnp.arange(bins_total, dtype=jnp.int32) >= plane_bin[plane_id]).astype(jnp.float32)
        convergence = convergence + weights[:, None, None] * plane_map
    spectrum = jnp.fft.fft2(convergence)
    first_factor, second_factor = shear_factors(wave_numbers(grid_cells)[:, None], wave_numbers(grid_cells)[None, :])
    kernel = lax.complex(first_factor, second_factor)
    field = jnp.fft.ifft2(kernel[None] * spectrum)
    return jnp.stack([jnp.real(field), jnp.imag(field)]).astype(jnp.float32)
```

```python
import math
import numpy as np
import jax
import jax.numpy as jnp
from jax import lax
from jax.sharding import PartitionSpec as P
from jax.experimental import pallas as pl
from jax.experimental.pallas import tpu as pltpu

BF = jnp.bfloat16
F32 = jnp.float32
N = 2048
HALF = 1024


def split_const(table):
    table = table.astype(np.float32)
    high = table.astype(BF)
    return high, (table - high.astype(np.float32)).astype(BF)


def tables():
    n2 = np.arange(128)
    k2p = np.arange(64)
    angle = 2.0 * np.pi * np.outer(n2, k2p) / 128.0
    cos, sin = np.cos(angle).reshape(128, 4, 16), np.sin(angle).reshape(128, 4, 16)
    first = np.concatenate([np.stack([cos, -sin], 2), np.stack([sin, cos], 2)], 0).reshape(256, 128)
    angle = 2.0 * np.pi * np.outer(n2, n2) / 128.0
    cos, sin = np.cos(angle), np.sin(angle)
    second = np.block([[cos, -sin], [sin, cos]])
    order = np.arange(128).reshape(64, 2).T.reshape(-1)
    back = np.block([[cos[:, order], sin[:, order]], [-sin[:, order], cos[:, order]]]) / N
    angle = 2.0 * np.pi * np.outer(k2p, n2) / 128.0
    cos, sin = np.cos(angle).reshape(4, 16, 128), np.sin(angle).reshape(4, 16, 128)
    final = np.concatenate([np.stack([cos, -sin], 1), np.stack([sin, cos], 1)], 3).reshape(128, 256) * (2.0 / N)
    swap = np.zeros((128, 128))
    swap[order, np.arange(128)] = 1.0
    angle = 2.0 * np.pi * np.outer(np.arange(16), n2) / N
    plain = np.concatenate([np.cos(angle), np.sin(angle)], 0).astype(np.float32)
    mixed = np.concatenate([np.cos(angle[:, order]), np.sin(angle[:, order])], 0).astype(np.float32)
    return first, second, back, final, swap, plain, mixed


def add(a, b):
    return b if a is None else a if b is None else a + b


def sub(a, b):
    return a if b is None else -b if a is None else a - b


def turn(value, numer, denom, sign):
    re, im = value
    eighth = (8 * numer // denom) if (8 * numer) % denom == 0 else None
    if eighth == 0:
        return value
    if eighth == 2:
        if sign == 1:
            return (None if im is None else -im, re)
        return (im, -re)
    c, s = math.cos(2 * math.pi * numer / denom), sign * math.sin(2 * math.pi * numer / denom)
    if im is None:
        return (re * c, re * s)
    if re is None:
        return (im * -s, im * c)
    return (re * c - im * s, re * s + im * c)


def short_dft(values, sign, real_out=False):
    n = len(values)
    if n == 1:
        return values
    even = short_dft(values[0::2], sign)
    odd = short_dft(values[1::2], sign)
    low, high = [], []
    for k in range(n // 2):
        t = turn(odd[k], k, n, sign)
        e = even[k]
        low.append((add(e[0], t[0]), None if real_out else add(e[1], t[1])))
        high.append((sub(e[0], t[0]), None if real_out else sub(e[1], t[1])))
    return low + high


def dot(a, b):
    return lax.dot_general(a, b, (((1,), (0,)), ((), ())), preferred_element_type=F32)


def split(x):
    high = x.astype(BF)
    return high, (x - high.astype(F32)).astype(BF)


def dot3(x, high, low):
    xh, xl = split(x)
    return dot(xh, high) + (dot(xl, high) + dot(xh, low))


def iota(shape, dim):
    return lax.broadcasted_iota(jnp.int32, shape, dim)


def wrapped(p):
    return jnp.where(p >= 1.0 * N, p - 1.0 * N, p)


def block_swap(tiles, roll):
    block = iota((8, 128), 1) // 32
    turned = {(i, d): (roll(tiles[i], 32 * d) if d else tiles[i]) for i in range(4) for d in range(4)}
    out = []
    for q in range(4):
        acc = turned[(0, (0 - q) % 4)]
        for i in range(1, 4):
            acc = jnp.where(block == i, turned[(i, (i - q) % 4)], acc)
        out.append(acc)
    return out


def columns_body(dens, pos, high, low, twid, roll, emit):
    r, c = iota((32, 32), 0), iota((32, 32), 1)
    perm = jnp.where(c == 4 * (r % 8) + r // 8, 1.0, 0.0).astype(BF)
    dens_f = dot(perm, dens)
    dens_p = dens_f.astype(BF)
    left = jnp.concatenate([dens_p[:, 256 * a : 256 * (a + 1)] for a in range(8)], axis=0)
    following = [dens_f[:, (256 * (a + 1)) % N : (256 * (a + 1)) % N + 1] for a in range(8)]
    cell = iota((256, 256), 0).astype(F32)
    tiles = []
    for v in range(8):
        p = wrapped(pos[:, 256 * v : 256 * (v + 1)])
        group = jnp.floor(p * (1.0 / 256.0))
        local = p - 256.0 * group
        table = jnp.maximum(1.0 - jnp.abs(cell - local), 0.0).astype(BF)
        edge = jnp.maximum(1.0 - jnp.abs(256.0 - local), 0.0).astype(BF).astype(F32)
        parts = dot(left, table)
        acc, nxt = parts[0:32], jnp.broadcast_to(following[0], (32, 256))
        for a in range(1, 8):
            hit = group == 1.0 * a
            acc = jnp.where(hit, parts[32 * a : 32 * (a + 1)], acc)
            nxt = jnp.where(hit, following[a], nxt)
        acc = acc + edge * nxt
        tiles += [acc[:, :128], acc[:, 128:]]
    freq = short_dft([(t, None) for t in tiles], -1)
    sign = jnp.where(iota((32, 128), 1) % 2 == 0, 1.0, -1.0)
    nyquist = jnp.sum(freq[0][0] * sign, axis=1, keepdims=True)
    for m in range(16):
        re, im = freq[m]
        if m == 0:
            zr, zi = re, jnp.zeros_like(re)
        else:
            co, si = twid[m : m + 1], twid[16 + m : 17 + m]
            im = jnp.zeros_like(re) if im is None else im
            zr, zi = re * co + im * si, im * co - re * si
        out = dot3(jnp.concatenate([zr, zi], axis=1), high, low)
        if m == 0:
            out = jnp.where(iota((32, 128), 1) == 16, nyquist, out)
        emit(m, jnp.concatenate(block_swap([out[8 * i : 8 * i + 8] for i in range(4)], roll), axis=0).astype(BF))


def rows_body(got, pos, trans, high2, low2, high3, low3, swap, twid, twid_mixed, roll, emit):
    k1p, q = trans // 4, trans % 4
    turned = got.astype(F32).T
    left = jnp.concatenate([turned, roll(turned[0:32], 511)], axis=0).astype(BF)
    cell = iota((512, 256), 0).astype(F32)
    tiles = []
    for u in range(8):
        p = wrapped(pos[:, 256 * u : 256 * (u + 1)])
        group = jnp.floor(p * 0.25)
        local = p - 4.0 * group
        table = jnp.where(cell == group, 1.0, 0.0).astype(BF)
        parts = dot(left, table)
        acc = None
        for s in range(5):
            weight = jnp.maximum(1.0 - jnp.abs(local - 1.0 * s), 0.0).astype(BF).astype(F32)
            acc = add(acc, weight * parts[32 * s : 32 * (s + 1)])
        tiles += [acc[:, :128], acc[:, 128:]]
    first = (iota((16, 128), 0) == 0) & (trans == 0)
    flat = [t[0:8] for t in tiles]
    total = flat[0]
    for t in flat[1:]:
        total = total + t
    mean = jnp.sum(total, axis=1, keepdims=True) * (1.0 / N)
    flat = dot(jnp.concatenate([t - mean for t in flat], axis=0).astype(BF), swap)
    values = []
    for t in tiles:
        re, im = t[0:16], t[16:32]
        values.append((jnp.where(first, im, re), jnp.where(first, 0.0, im)))
    freq = short_dft(values, -1)
    kappa = iota((16, 128), 0)
    lane = iota((16, 128), 1)
    k2 = 256 * q + 16 * kappa + k1p
    k2 = jnp.where(first, -HALF, k2)
    back = []
    for m in range(16):
        re, im = freq[m]
        if m:
            co, si = twid[m : m + 1], twid[16 + m : 17 + m]
            re, im = re * co + im * si, im * co - re * si
        out = dot3(jnp.concatenate([re, im], axis=1), high2, low2)
        xr, xi = out[:, :128], out[:, 128:]
        k1 = m + 16 * lane
        k1 = jnp.where(k1 >= HALF, k1 - N, k1)
        special = (k1 == -HALF) != (k2 == -HALF)
        w1, w2 = k1.astype(F32), k2.astype(F32)
        inverse = 1.0 / jnp.maximum(w1 * w1 + w2 * w2, 1.0)
        ka = (w1 * w1 - w2 * w2) * inverse
        kb = 2.0 * w1 * w2 * inverse
        odd = jnp.where(special, kb, 0.0)
        even = jnp.where(special, 0.0, kb)
        vr = jnp.concatenate([ka * xr - odd * xi, even * xr], axis=0)
        vi = jnp.concatenate([ka * xi + odd * xr, even * xi], axis=0)
        out = dot3(jnp.concatenate([vr, vi], axis=1), high3, low3)
        re, im = out[:, :128], out[:, 128:]
        if m:
            co, si = twid_mixed[m : m + 1], twid_mixed[16 + m : 17 + m]
            re, im = re * co - im * si, im * co + re * si
        back.append((re, im))
    space = short_dft(back, 1)
    low_half = iota((64, 128), 1) < 64
    zero = jnp.zeros((8, 128), F32)
    stacked = []
    for n in range(16):
        re, im = space[n]
        real0 = jnp.concatenate([flat[8 * n : 8 * n + 8], zero], axis=0)
        r0, r1, i0, i1 = re[0:16], re[16:32], im[0:16], im[16:32]
        stacked.append(
            jnp.concatenate(
                [
                    jnp.where(first, real0, r0),
                    jnp.where(first, r0, i0),
                    jnp.where(first, 0.0, r1),
                    jnp.where(first, r1, i1),
                ],
                axis=0,
            )
        )
    for m in range(8):
        a, b = stacked[2 * m], stacked[2 * m + 1]
        top = jnp.where(low_half, a, roll(b, 64))
        bottom = jnp.where(low_half, roll(a, 64), b)
        emit(m, jnp.concatenate([top, bottom], axis=0).T.astype(BF))


def final_body(load, weight, high, low, twid, roll, emit):
    row, col = iota((64, 128), 0), iota((64, 128), 1)
    slot = (iota((1, 128), 1) // 2) % 8
    mix = jnp.zeros((64, 128), F32)
    for b in range(4):
        line = jnp.zeros((1, 128), F32)
        for s in range(8):
            line = jnp.where(slot == s, weight(b, s), line)
        mix = jnp.where((row // 2) % 4 == b, line, mix)
    mix = jnp.where((row // 8 == col // 16) & (row % 2 == col % 2), mix, 0.0)
    mix_high, mix_low = split(mix)
    lane = iota((32, 128), 1)
    sign = jnp.where(lane % 2 == 0, 1.0, -1.0)
    values = []
    for block in range(8):
        got = load(block)
        summed = dot(mix_high, got) + dot(mix_low, got)
        for half in range(2):
            m = 2 * block + half
            base = 32 * half
            line = jnp.concatenate(block_swap([summed[base + 8 * i : base + 8 * i + 8] for i in range(4)], roll), axis=0)
            if m == 0:
                nyquist = line[:, 16:17]
                line = jnp.where(lane == 0, 0.5 * line, line)
            out = dot3(line, high, low)
            re, im = out[:, :128], out[:, 128:]
            if m == 0:
                values.append((re + (nyquist * (1.0 / N)) * sign, None))
            else:
                co, si = twid[m : m + 1], twid[16 + m : 17 + m]
                values.append((re * co - im * si, im * co + re * si))
    done = short_dft(values, 1, real_out=True)
    for n in range(16):
        emit(n, done[n][0])


def rolled(x, shift):
    return pltpu.roll(x, shift, 1)


def columns_kernel(plane_ref, dens_ref, pos_ref, high_ref, low_ref, twid_ref, out_ref):
    plane = plane_ref[lax.axis_index("los")]

    def emit(m, value):
        out_ref[32 * m : 32 * m + 32, :] = value

    columns_body(dens_ref[0], pos_ref[pl.ds(plane, 1), :], high_ref[...], low_ref[...], twid_ref, rolled, emit)


def rows_kernel(plane_ref, got_ref, pos_ref, high2_ref, low2_ref, high3_ref, low3_ref, swap_ref, twid_ref, mixed_ref, out_ref):
    plane = plane_ref[lax.axis_index("los")]

    def emit(m, value):
        out_ref[128 * m : 128 * m + 128, :] = value

    rows_body(
        got_ref[...],
        pos_ref[pl.ds(plane, 1), :],
        lax.axis_index("trans"),
        high2_ref[...],
        low2_ref[...],
        high3_ref[...],
        low3_ref[...],
        swap_ref[...],
        twid_ref,
        mixed_ref,
        rolled,
        emit,
    )


def final_kernel(plane_ref, bin_ref, eff_ref, got_ref, high_ref, low_ref, twid_ref, out_ref, wide_ref):
    def weight(b, s):
        plane = plane_ref[s]
        return jnp.where(b >= bin_ref[plane], eff_ref[b, plane], 0.0)

    def emit(n, value):
        for g in range(4):
            jl, comp = g // 2, g % 2
            wide_ref[n, pl.ds(16 * comp + jl, 8, stride=2), :] = value[8 * g : 8 * g + 8]

    final_body(
        lambda block: got_ref[128 * block : 128 * block + 128, :], weight, high_ref[...], low_ref[...], twid_ref, rolled, emit
    )
    for n in range(16):
        for comp in range(2):
            for b in range(4):
                base = 16 * comp + 4 * b
                out_ref[comp, b, :, 128 * n : 128 * n + 128] = wide_ref[n, base : base + 4, :]


def call(kernel, shape, dtype, scalars, arrays, scratch=()):
    smem = pl.BlockSpec(memory_space=pltpu.SMEM)
    vmem = pl.BlockSpec(memory_space=pltpu.VMEM)
    return pl.pallas_call(
        kernel,
        out_shape=jax.ShapeDtypeStruct(shape, dtype),
        in_specs=[smem] * len(scalars) + [vmem] * len(arrays),
        out_specs=vmem,
        scratch_shapes=scratch,
    )(*scalars, *arrays)


def body(density, row_pos, col_pos, plane_of_slot, plane_bin, efficiency):
    first, second, back, final, swap, plain, mixed = tables()
    swap = swap.astype(BF)
    sent = call(
        columns_kernel, (512, 128), BF, [plane_of_slot], [density, col_pos, *split_const(first), plain]
    )
    got = lax.all_to_all(sent.reshape(64, 8, 128), "trans", split_axis=0, concat_axis=0, tiled=True)
    sent = call(
        rows_kernel,
        (1024, 128),
        BF,
        [plane_of_slot],
        [got.reshape(512, 128), row_pos, *split_const(second), *split_const(back), swap, plain, mixed],
    )
    got = lax.all_to_all(sent.reshape(512, 2, 128), ("trans", "los"), split_axis=0, concat_axis=0, tiled=True)
    return call(
        final_kernel,
        (2, 4, 4, N),
        F32,
        [plane_of_slot, plane_bin, efficiency],
        [got.reshape(1024, 128), *split_const(final), plain],
        [pltpu.VMEM((16, 32, 128), F32)],
    )


def solution(mesh):
    placed = (P("los", "trans", None), P(), P(), P(), P(), P())
    return jax.shard_map(
        body,
        mesh=mesh,
        in_specs=placed,
        out_specs=P(None, None, ("trans", "los"), None),
        check_vma=False,
    )
```

```python
import math
import numpy as np
import jax
import jax.numpy as jnp
from jax import lax
from jax.sharding import PartitionSpec as P
from jax.experimental import pallas as pl
from jax.experimental.pallas import tpu as pltpu

BF = jnp.bfloat16
F32 = jnp.float32
N = 2048
HALF = 1024


def split_const(table):
    table = table.astype(np.float32)
    high = table.astype(BF)
    return high, (table - high.astype(np.float32)).astype(BF)


def tables():
    n2 = np.arange(128)
    k2p = np.arange(64)
    angle = 2.0 * np.pi * np.outer(n2, k2p) / 128.0
    cos, sin = np.cos(angle).reshape(128, 4, 16), np.sin(angle).reshape(128, 4, 16)
    first = np.concatenate([np.stack([cos, -sin], 2), np.stack([sin, cos], 2)], 0).reshape(256, 128)
    angle = 2.0 * np.pi * np.outer(n2, n2) / 128.0
    cos, sin = np.cos(angle), np.sin(angle)
    second = np.block([[cos, -sin], [sin, cos]])
    order = np.arange(128).reshape(64, 2).T.reshape(-1)
    back = np.block([[cos[:, order], sin[:, order]], [-sin[:, order], cos[:, order]]]) / N
    angle = 2.0 * np.pi * np.outer(k2p, n2) / 128.0
    cos, sin = np.cos(angle).reshape(4, 16, 128), np.sin(angle).reshape(4, 16, 128)
    final = np.concatenate([np.stack([cos, -sin], 1), np.stack([sin, cos], 1)], 3).reshape(128, 256) * (2.0 / N)
    swap = np.zeros((128, 128))
    swap[order, np.arange(128)] = 1.0
    angle = 2.0 * np.pi * np.outer(np.arange(16), n2) / N
    plain = np.concatenate([np.cos(angle), np.sin(angle)], 0).astype(np.float32)
    mixed = np.concatenate([np.cos(angle[:, order]), np.sin(angle[:, order])], 0).astype(np.float32)
    return first, second, back, final, swap, plain, mixed


def add(a, b):
    return b if a is None else a if b is None else a + b


def sub(a, b):
    return a if b is None else -b if a is None else a - b


def turn(value, numer, denom, sign):
    re, im = value
    eighth = (8 * numer // denom) if (8 * numer) % denom == 0 else None
    if eighth == 0:
        return value
    if eighth == 2:
        if sign == 1:
            return (None if im is None else -im, re)
        return (im, -re)
    c, s = math.cos(2 * math.pi * numer / denom), sign * math.sin(2 * math.pi * numer / denom)
    if im is None:
        return (re * c, re * s)
    if re is None:
        return (im * -s, im * c)
    return (re * c - im * s, re * s + im * c)


def short_dft(values, sign, real_out=False):
    n = len(values)
    if n == 1:
        return values
    even = short_dft(values[0::2], sign)
    odd = short_dft(values[1::2], sign)
    low, high = [], []
    for k in range(n // 2):
        t = turn(odd[k], k, n, sign)
        e = even[k]
        low.append((add(e[0], t[0]), None if real_out else add(e[1], t[1])))
        high.append((sub(e[0], t[0]), None if real_out else sub(e[1], t[1])))
    return low + high


def dot(a, b):
    return lax.dot_general(a, b, (((1,), (0,)), ((), ())), preferred_element_type=F32)


def split(x):
    high = x.astype(BF)
    return high, (x - high.astype(F32)).astype(BF)


def dot3(x, high, low):
    xh, xl = split(x)
    return dot(xh, high) + (dot(xl, high) + dot(xh, low))


def iota(shape, dim):
    return lax.broadcasted_iota(jnp.int32, shape, dim)


def wrapped(p):
    return jnp.where(p >= 1.0 * N, p - 1.0 * N, p)


def block_swap(tiles, roll):
    block = iota((8, 128), 1) // 32
    turned = {(i, d): (roll(tiles[i], 32 * d) if d else tiles[i]) for i in range(4) for d in range(4)}
    out = []
    for q in range(4):
        acc = turned[(0, (0 - q) % 4)]
        for i in range(1, 4):
            acc = jnp.where(block == i, turned[(i, (i - q) % 4)], acc)
        out.append(acc)
    return out


def columns_body(dens, pos, high, low, twid, roll, emit):
    r, c = iota((32, 32), 0), iota((32, 32), 1)
    perm = jnp.where(c == 4 * (r % 8) + r // 8, 1.0, 0.0).astype(BF)
    dens_f = dot(perm, dens)
    dens_p = dens_f.astype(BF)
    left = jnp.concatenate([dens_p[:, 256 * a : 256 * (a + 1)] for a in range(8)], axis=0)
    following = [dens_f[:, (256 * (a + 1)) % N : (256 * (a + 1)) % N + 1] for a in range(8)]
    cell = iota((256, 256), 0).astype(F32)
    tiles = []
    for v in range(8):
        p = wrapped(pos[:, 256 * v : 256 * (v + 1)])
        group = jnp.floor(p * (1.0 / 256.0))
        local = p - 256.0 * group
        table = jnp.maximum(1.0 - jnp.abs(cell - local), 0.0).astype(BF)
        edge = jnp.maximum(1.0 - jnp.abs(256.0 - local), 0.0).astype(BF).astype(F32)
        parts = dot(left, table)
        acc, nxt = parts[0:32], jnp.broadcast_to(following[0], (32, 256))
        for a in range(1, 8):
            hit = group == 1.0 * a
            acc = jnp.where(hit, parts[32 * a : 32 * (a + 1)], acc)
            nxt = jnp.where(hit, following[a], nxt)
        acc = acc + edge * nxt
        tiles += [acc[:, :128], acc[:, 128:]]
    freq = short_dft([(t, None) for t in tiles], -1)
    sign = jnp.where(iota((32, 128), 1) % 2 == 0, 1.0, -1.0)
    nyquist = jnp.sum(freq[0][0] * sign, axis=1, keepdims=True)
    for m in range(16):
        re, im = freq[m]
        if m == 0:
            zr, zi = re, jnp.zeros_like(re)
        else:
            co, si = twid[m : m + 1], twid[16 + m : 17 + m]
            im = jnp.zeros_like(re) if im is None else im
            zr, zi = re * co + im * si, im * co - re * si
        out = dot3(jnp.concatenate([zr, zi], axis=1), high, low)
        if m == 0:
            out = jnp.where(iota((32, 128), 1) == 16, nyquist, out)
        emit(m, jnp.concatenate(block_swap([out[8 * i : 8 * i + 8] for i in range(4)], roll), axis=0).astype(BF))


def rows_body(got, pos, trans, high2, low2, high3, low3, swap, twid, twid_mixed, roll, emit):
    k1p, q = trans // 4, trans % 4
    turned = got.astype(F32).T
    left = jnp.concatenate([turned, roll(turned[0:32], 511)], axis=0).astype(BF)
    cell = iota((512, 256), 0).astype(F32)
    tiles = []
    for u in range(8):
        p = wrapped(pos[:, 256 * u : 256 * (u + 1)])
        group = jnp.floor(p * 0.25)
        local = p - 4.0 * group
        table = jnp.where(cell == group, 1.0, 0.0).astype(BF)
        parts = dot(left, table)
        acc = None
        for s in range(5):
            weight = jnp.maximum(1.0 - jnp.abs(local - 1.0 * s), 0.0).astype(BF).astype(F32)
            acc = add(acc, weight * parts[32 * s : 32 * (s + 1)])
        tiles += [acc[:, :128], acc[:, 128:]]
    first = (iota((16, 128), 0) == 0) & (trans == 0)
    flat = [t[0:8] for t in tiles]
    total = flat[0]
    for t in flat[1:]:
        total = total + t
    mean = jnp.sum(total, axis=1, keepdims=True) * (1.0 / N)
    flat = dot(jnp.concatenate([t - mean for t in flat], axis=0).astype(BF), swap)
    values = []
    for t in tiles:
        re, im = t[0:16], t[16:32]
        values.append((jnp.where(first, im, re), jnp.where(first, 0.0, im)))
    freq = short_dft(values, -1)
    kappa = iota((16, 128), 0)
    lane = iota((16, 128), 1)
    k2 = 256 * q + 16 * kappa + k1p
    k2 = jnp.where(first, -HALF, k2)
    back = []
    for m in range(16):
        re, im = freq[m]
        if m:
            co, si = twid[m : m + 1], twid[16 + m : 17 + m]
            re, im = re * co + im * si, im * co - re * si
        out = dot3(jnp.concatenate([re, im], axis=1), high2, low2)
        xr, xi = out[:, :128], out[:, 128:]
        k1 = m + 16 * lane
        k1 = jnp.where(k1 >= HALF, k1 - N, k1)
        special = (k1 == -HALF) != (k2 == -HALF)
        w1, w2 = k1.astype(F32), k2.astype(F32)
        inverse = 1.0 / jnp.maximum(w1 * w1 + w2 * w2, 1.0)
        ka = (w1 * w1 - w2 * w2) * inverse
        kb = 2.0 * w1 * w2 * inverse
        odd = jnp.where(special, kb, 0.0)
        even = jnp.where(special, 0.0, kb)
        vr = jnp.concatenate([ka * xr - odd * xi, even * xr], axis=0)
        vi = jnp.concatenate([ka * xi + odd * xr, even * xi], axis=0)
        out = dot3(jnp.concatenate([vr, vi], axis=1), high3, low3)
        re, im = out[:, :128], out[:, 128:]
        if m:
            co, si = twid_mixed[m : m + 1], twid_mixed[16 + m : 17 + m]
            re, im = re * co - im * si, im * co + re * si
        back.append((re, im))
    space = short_dft(back, 1)
    low_half = iota((64, 128), 1) < 64
    zero = jnp.zeros((8, 128), F32)
    stacked = []
    for n in range(16):
        re, im = space[n]
        real0 = jnp.concatenate([flat[8 * n : 8 * n + 8], zero], axis=0)
        r0, r1, i0, i1 = re[0:16], re[16:32], im[0:16], im[16:32]
        stacked.append(
            jnp.concatenate(
                [
                    jnp.where(first, real0, r0),
                    jnp.where(first, r0, i0),
                    jnp.where(first, 0.0, r1),
                    jnp.where(first, r1, i1),
                ],
                axis=0,
            )
        )
    for m in range(8):
        a, b = stacked[2 * m], stacked[2 * m + 1]
        top = jnp.where(low_half, a, roll(b, 64))
        bottom = jnp.where(low_half, roll(a, 64), b)
        emit(m, jnp.concatenate([top, bottom], axis=0).T.astype(BF))


def final_body(load, weight, high, low, twid, roll, emit):
    row, col = iota((64, 128), 0), iota((64, 128), 1)
    slot = (iota((1, 128), 1) // 2) % 8
    mix = jnp.zeros((64, 128), F32)
    for b in range(4):
        line = jnp.zeros((1, 128), F32)
        for s in range(8):
            line = jnp.where(slot == s, weight(b, s), line)
        mix = jnp.where((row // 2) % 4 == b, line, mix)
    mix = jnp.where((row // 8 == col // 16) & (row % 2 == col % 2), mix, 0.0)
    mix_high, mix_low = split(mix)
    lane = iota((32, 128), 1)
    sign = jnp.where(lane % 2 == 0, 1.0, -1.0)
    values = []
    for block in range(8):
        got = load(block)
        summed = dot(mix_high, got) + dot(mix_low, got)
        for half in range(2):
            m = 2 * block + half
            base = 32 * half
            line = jnp.concatenate(block_swap([summed[base + 8 * i : base + 8 * i + 8] for i in range(4)], roll), axis=0)
            if m == 0:
                nyquist = line[:, 16:17]
                line = jnp.where(lane == 0, 0.5 * line, line)
            out = dot3(line, high, low)
            re, im = out[:, :128], out[:, 128:]
            if m == 0:
                values.append((re + (nyquist * (1.0 / N)) * sign, None))
            else:
                co, si = twid[m : m + 1], twid[16 + m : 17 + m]
                values.append((re * co - im * si, im * co + re * si))
    done = short_dft(values, 1, real_out=True)
    for n in range(16):
        emit(n, done[n][0])


def rolled(x, shift):
    return pltpu.roll(x, shift, 1)


def columns_kernel(plane_ref, dens_ref, pos_ref, high_ref, low_ref, twid_ref, out_ref):
    plane = plane_ref[lax.axis_index("los")]

    def emit(m, value):
        out_ref[32 * m : 32 * m + 32, :] = value

    columns_body(dens_ref[0], pos_ref[pl.ds(plane, 1), :], high_ref[...], low_ref[...], twid_ref, rolled, emit)


def rows_kernel(plane_ref, got_ref, pos_ref, high2_ref, low2_ref, high3_ref, low3_ref, swap_ref, twid_ref, mixed_ref, out_ref):
    plane = plane_ref[lax.axis_index("los")]

    def emit(m, value):
        out_ref[128 * m : 128 * m + 128, :] = value

    rows_body(
        got_ref[...],
        pos_ref[pl.ds(plane, 1), :],
        lax.axis_index("trans"),
        high2_ref[...],
        low2_ref[...],
        high3_ref[...],
        low3_ref[...],
        swap_ref[...],
        twid_ref,
        mixed_ref,
        rolled,
        emit,
    )


def final_kernel(plane_ref, bin_ref, eff_ref, got_ref, high_ref, low_ref, twid_ref, out_ref, wide_ref):
    def weight(b, s):
        plane = plane_ref[s]
        return jnp.where(b >= bin_ref[plane], eff_ref[b, plane], 0.0)

    def emit(n, value):
        for g in range(4):
            jl, comp = g // 2, g % 2
            wide_ref[n, pl.ds(16 * comp + jl, 8, stride=2), :] = value[8 * g : 8 * g + 8]

    final_body(
        lambda block: got_ref[128 * block : 128 * block + 128, :], weight, high_ref[...], low_ref[...], twid_ref, rolled, emit
    )
    for n in range(16):
        for comp in range(2):
            for b in range(4):
                base = 16 * comp + 4 * b
                out_ref[comp, b, :, 128 * n : 128 * n + 128] = wide_ref[n, base : base + 4, :]


def call(kernel, shape, dtype, scalars, arrays, scratch=()):
    smem = pl.BlockSpec(memory_space=pltpu.SMEM)
    vmem = pl.BlockSpec(memory_space=pltpu.VMEM)
    return pl.pallas_call(
        kernel,
        out_shape=jax.ShapeDtypeStruct(shape, dtype),
        in_specs=[smem] * len(scalars) + [vmem] * len(arrays),
        out_specs=vmem,
        scratch_shapes=scratch,
        compiler_params=pltpu.CompilerParams(vmem_limit_bytes=16 << 20),
    )(*scalars, *arrays)


def body(density, row_pos, col_pos, plane_of_slot, plane_bin, efficiency):
    first, second, back, final, swap, plain, mixed = tables()
    swap = swap.astype(BF)
    sent = call(
        columns_kernel, (512, 128), BF, [plane_of_slot], [density, col_pos, *split_const(first), plain]
    )
    got = lax.all_to_all(sent.reshape(64, 8, 128), "trans", split_axis=0, concat_axis=0, tiled=True)
    sent = call(
        rows_kernel,
        (1024, 128),
        BF,
        [plane_of_slot],
        [got.reshape(512, 128), row_pos, *split_const(second), *split_const(back), swap, plain, mixed],
    )
    got = lax.all_to_all(sent.reshape(512, 2, 128), ("trans", "los"), split_axis=0, concat_axis=0, tiled=True)
    return call(
        final_kernel,
        (2, 4, 4, N),
        F32,
        [plane_of_slot, plane_bin, efficiency],
        [got.reshape(1024, 128), *split_const(final), plain],
        [pltpu.VMEM((16, 32, 128), F32)],
    )


def solution(mesh):
    placed = (P("los", "trans", None), P(), P(), P(), P(), P())
    return jax.shard_map(
        body,
        mesh=mesh,
        in_specs=placed,
        out_specs=P(None, None, ("trans", "los"), None),
        check_vma=False,
    )
```

```python
import math
import numpy as np
import jax
import jax.numpy as jnp
from jax import lax
from jax.sharding import PartitionSpec as P
from jax.experimental import pallas as pl
from jax.experimental.pallas import tpu as pltpu

BF = jnp.bfloat16
F32 = jnp.float32
N = 2048
HALF = 1024


def pair(table):
    table = table.astype(np.float32)
    high = table.astype(BF)
    return np.concatenate([high, (table - high.astype(np.float32)).astype(BF)], axis=0)


def tables():
    n2 = np.arange(128)
    k2p = np.arange(64)
    angle = 2.0 * np.pi * np.outer(n2, k2p) / 128.0
    cos, sin = np.cos(angle).reshape(128, 4, 16), np.sin(angle).reshape(128, 4, 16)
    first = np.concatenate([np.stack([cos, -sin], 2), np.stack([sin, cos], 2)], 0).reshape(256, 128)
    angle = 2.0 * np.pi * np.outer(n2, n2) / 128.0
    cos, sin = np.cos(angle), np.sin(angle)
    second = np.block([[cos, -sin], [sin, cos]])
    order = np.arange(128).reshape(64, 2).T.reshape(-1)
    back = np.block([[cos[:, order], sin[:, order]], [-sin[:, order], cos[:, order]]]) / N
    angle = 2.0 * np.pi * np.outer(k2p, n2) / 128.0
    cos, sin = np.cos(angle).reshape(4, 16, 128), np.sin(angle).reshape(4, 16, 128)
    final = np.concatenate([np.stack([cos, -sin], 1), np.stack([sin, cos], 1)], 3).reshape(128, 256) * (2.0 / N)
    swap = np.zeros((128, 128))
    swap[order, np.arange(128)] = 1.0
    angle = 2.0 * np.pi * np.outer(np.arange(16), n2) / N
    plain = np.concatenate([np.cos(angle), np.sin(angle)], 0).astype(np.float32)
    mixed = np.concatenate([np.cos(angle[:, order]), np.sin(angle[:, order])], 0).astype(np.float32)
    return first, second, back, final, swap, plain, mixed


def add(a, b):
    return b if a is None else a if b is None else a + b


def sub(a, b):
    return a if b is None else -b if a is None else a - b


def turn(value, numer, denom, sign):
    re, im = value
    eighth = (8 * numer // denom) if (8 * numer) % denom == 0 else None
    if eighth == 0:
        return value
    if eighth == 2:
        if sign == 1:
            return (None if im is None else -im, re)
        return (im, -re)
    c, s = math.cos(2 * math.pi * numer / denom), sign * math.sin(2 * math.pi * numer / denom)
    if im is None:
        return (re * c, re * s)
    if re is None:
        return (im * -s, im * c)
    return (re * c - im * s, re * s + im * c)


def short_dft(values, sign, real_out=False):
    n = len(values)
    if n == 1:
        return values
    even = short_dft(values[0::2], sign)
    odd = short_dft(values[1::2], sign)
    low, high = [], []
    for k in range(n // 2):
        t = turn(odd[k], k, n, sign)
        e = even[k]
        low.append((add(e[0], t[0]), None if real_out else add(e[1], t[1])))
        high.append((sub(e[0], t[0]), None if real_out else sub(e[1], t[1])))
    return low + high


def dot(a, b):
    return lax.dot_general(a, b, (((1,), (0,)), ((), ())), preferred_element_type=F32)


def split(x):
    high = x.astype(BF)
    return high, (x - high.astype(F32)).astype(BF)


def dot3(x, table):
    high, low = split(x)
    top = table[: x.shape[1]]
    return dot(jnp.concatenate([high, low, high], axis=1), jnp.concatenate([top, table], axis=0))


def iota(shape, dim):
    return lax.broadcasted_iota(jnp.int32, shape, dim)


def wrapped(p):
    return jnp.where(p >= 1.0 * N, p - 1.0 * N, p)


def block_swap(tiles, roll):
    block = iota((8, 128), 1) // 32
    turned = {(i, d): (roll(tiles[i], 32 * d) if d else tiles[i]) for i in range(4) for d in range(4)}
    out = []
    for q in range(4):
        acc = turned[(0, (0 - q) % 4)]
        for i in range(1, 4):
            acc = jnp.where(block == i, turned[(i, (i - q) % 4)], acc)
        out.append(acc)
    return out


def mixing(weight):
    row, col = iota((64, 128), 0), iota((64, 128), 1)
    slot = (iota((1, 128), 1) // 2) % 8
    mix = jnp.zeros((64, 128), F32)
    for b in range(4):
        line = jnp.zeros((1, 128), F32)
        for s in range(8):
            line = jnp.where(slot == s, weight(b, s), line)
        mix = jnp.where((row // 2) % 4 == b, line, mix)
    mix = jnp.where((row // 8 == col // 16) & (row % 2 == col % 2), mix, 0.0)
    return jnp.concatenate(split(mix), axis=0)


def columns_body(dens, pos, table_of, twid, roll, emit):
    r, c = iota((32, 32), 0), iota((32, 32), 1)
    perm = jnp.where(c == 4 * (r % 8) + r // 8, 1.0, 0.0).astype(BF)
    dens_f = dot(perm, dens)
    dens_p = dens_f.astype(BF)
    left = jnp.concatenate([dens_p[:, 256 * a : 256 * (a + 1)] for a in range(8)], axis=0)
    following = [dens_f[:, (256 * (a + 1)) % N : (256 * (a + 1)) % N + 1] for a in range(8)]
    cell = iota((256, 256), 0).astype(F32).astype(BF)
    zero = jnp.zeros((256, 256), BF)
    tiles = []
    for v in range(8):
        p = wrapped(pos[:, 256 * v : 256 * (v + 1)])
        group = jnp.floor(p * (1.0 / 256.0))
        local = p - 256.0 * group
        base = jnp.floor(local)
        here = (1.0 - (local - base)).astype(BF)
        there = (1.0 - (base + 1.0 - local)).astype(BF)
        table = jnp.where(cell == base.astype(BF), here, jnp.where(cell == (base + 1.0).astype(BF), there, zero))
        edge = jnp.where(base == 255.0, there.astype(F32), 0.0)
        parts = dot(left, table)
        acc, nxt = parts[0:32], jnp.broadcast_to(following[0], (32, 256))
        for a in range(1, 8):
            hit = group == 1.0 * a
            acc = jnp.where(hit, parts[32 * a : 32 * (a + 1)], acc)
            nxt = jnp.where(hit, following[a], nxt)
        acc = acc + edge * nxt
        tiles += [acc[:, :128], acc[:, 128:]]
    freq = short_dft([(t, None) for t in tiles], -1)
    lane, row = iota((32, 128), 1), iota((32, 128), 0)
    sign = jnp.where(lane % 2 == 0, 1.0, -1.0)
    nyquist = jnp.sum(freq[0][0] * sign, axis=1, keepdims=True)
    turned = []
    for m in range(16):
        re, im = freq[m]
        im = jnp.zeros_like(re) if im is None else im
        if m:
            co, si = twid[m : m + 1], twid[16 + m : 17 + m]
            re, im = re * co + im * si, im * co - re * si
        turned.append(jnp.concatenate([re, im], axis=1))
    result = dot3(jnp.concatenate(turned, axis=0), table_of())
    for m in range(16):
        out = result[32 * m : 32 * m + 32]
        if m == 0:
            base = out[0:1, 0:1].astype(BF).astype(F32)
            out = jnp.where((lane == 0) & (row > 0), out - base, jnp.where(lane == 16, nyquist, out))
        emit(m, jnp.concatenate(block_swap([out[8 * i : 8 * i + 8] for i in range(4)], roll), axis=0).astype(BF))


def rows_body(got, pos, trans, ready, twid, twid_mixed, roll, emit):
    k1p, q = trans // 4, trans % 4
    turned = got.astype(F32).T
    marked = (iota((8, 512), 0) == 0) & (iota((8, 512), 1) % 8 == 0) & (trans == 0)
    base = jnp.where(marked, turned[0:8], 0.0)
    turned = jnp.concatenate([jnp.where(marked, 0.0, turned[0:8]), turned[8:]], axis=0)
    for step in (1, 2, 4):
        base = base + roll(base, step)
    left = jnp.concatenate([turned, roll(turned[0:32], 511), base, roll(base, 511)], axis=0).astype(BF)
    cell = iota((256, 256), 0).astype(F32).astype(BF)
    one, zero = jnp.ones((256, 256), BF), jnp.zeros((256, 256), BF)
    tiles = []
    for u in range(8):
        p = wrapped(pos[:, 256 * u : 256 * (u + 1)])
        group = jnp.floor(p * 0.25)
        local = p - 4.0 * group
        table = jnp.concatenate(
            [jnp.where(cell == group.astype(BF), one, zero), jnp.where(cell == (group - 256.0).astype(BF), one, zero)], axis=0
        )
        parts = dot(left, table)
        acc = total = None
        for s in range(5):
            weight = jnp.maximum(1.0 - jnp.abs(local - 1.0 * s), 0.0).astype(BF).astype(F32)
            acc = add(acc, weight * parts[32 * s : 32 * (s + 1)])
            if s < 4:
                total = add(total, weight)
        extra = total * parts[160:168] + weight * parts[168:176]
        acc = jnp.concatenate([acc[0:8] + extra, acc[8:32]], axis=0)
        tiles += [acc[:, :128], acc[:, 128:]]
    table2, table3, swap = ready()
    first = (iota((16, 128), 0) == 0) & (trans == 0)
    flat = [t[0:8] for t in tiles]
    total = flat[0]
    for t in flat[1:]:
        total = total + t
    mean = jnp.sum(total, axis=1, keepdims=True) * (1.0 / N)
    flat = dot(jnp.concatenate([t - mean for t in flat], axis=0).astype(BF), swap)
    values = []
    for t in tiles:
        re, im = t[0:16], t[16:32]
        values.append((jnp.where(first, im, re), jnp.where(first, 0.0, im)))
    freq = short_dft(values, -1)
    turned = []
    for m in range(16):
        re, im = freq[m]
        if m:
            co, si = twid[m : m + 1], twid[16 + m : 17 + m]
            re, im = re * co + im * si, im * co - re * si
        turned.append(jnp.concatenate([re, im], axis=1))
    spectrum = dot3(jnp.concatenate(turned, axis=0), table2)
    kappa = iota((16, 128), 0)
    lane = iota((16, 128), 1)
    k2 = 256 * q + 16 * kappa + k1p
    k2 = jnp.where(first, -HALF, k2)
    w2 = k2.astype(F32)
    turned = []
    for m in range(16):
        xr, xi = spectrum[16 * m : 16 * m + 16, :128], spectrum[16 * m : 16 * m + 16, 128:]
        k1 = m + 16 * lane
        k1 = jnp.where(k1 >= HALF, k1 - N, k1)
        w1 = k1.astype(F32)
        inverse = 1.0 / jnp.maximum(w1 * w1 + w2 * w2, 1.0)
        ka = (w1 * w1 - w2 * w2) * inverse
        kb = 2.0 * w1 * w2 * inverse
        special = (k1 == -HALF) != (k2 == -HALF)
        odd = jnp.where(special, kb, 0.0)
        even = jnp.where(special, 0.0, kb)
        vr = jnp.concatenate([ka * xr - odd * xi, even * xr], axis=0)
        vi = jnp.concatenate([ka * xi + odd * xr, even * xi], axis=0)
        turned.append(jnp.concatenate([vr, vi], axis=1))
    result = dot3(jnp.concatenate(turned, axis=0), table3)
    back = []
    for m in range(16):
        re, im = result[32 * m : 32 * m + 32, :128], result[32 * m : 32 * m + 32, 128:]
        if m:
            co, si = twid_mixed[m : m + 1], twid_mixed[16 + m : 17 + m]
            re, im = re * co - im * si, im * co + re * si
        back.append((re, im))
    space = short_dft(back, 1)
    low_half = iota((64, 128), 1) < 64
    zero = jnp.zeros((8, 128), F32)
    stacked = []
    for n in range(16):
        re, im = space[n]
        real0 = jnp.concatenate([flat[8 * n : 8 * n + 8], zero], axis=0)
        r0, r1, i0, i1 = re[0:16], re[16:32], im[0:16], im[16:32]
        stacked.append(
            jnp.concatenate(
                [
                    jnp.where(first, real0, r0),
                    jnp.where(first, r0, i0),
                    jnp.where(first, 0.0, r1),
                    jnp.where(first, r1, i1),
                ],
                axis=0,
            )
        )
    for m in range(8):
        a, b = stacked[2 * m], stacked[2 * m + 1]
        top = jnp.where(low_half, a, roll(b, 64))
        bottom = jnp.where(low_half, roll(a, 64), b)
        emit(m, jnp.concatenate([top, bottom], axis=0).T.astype(BF))


def final_body(load, mix, table_of, twid, roll, emit):
    lane = iota((32, 128), 1)
    sign = jnp.where(lane % 2 == 0, 1.0, -1.0)
    lines = []
    for block in range(8):
        summed = dot(mix, load(block))
        summed = summed[0:64] + summed[64:128]
        for half in range(2):
            base = 32 * half
            line = jnp.concatenate(block_swap([summed[base + 8 * i : base + 8 * i + 8] for i in range(4)], roll), axis=0)
            if block == 0 and half == 0:
                nyquist = line[:, 16:17]
                line = jnp.where(lane == 0, 0.5 * line, line)
            lines.append(line)
    result = dot3(jnp.concatenate(lines, axis=0), table_of())
    values = []
    for m in range(16):
        re, im = result[32 * m : 32 * m + 32, :128], result[32 * m : 32 * m + 32, 128:]
        if m == 0:
            values.append((re + (nyquist * (1.0 / N)) * sign, None))
        else:
            co, si = twid[m : m + 1], twid[16 + m : 17 + m]
            values.append((re * co - im * si, im * co + re * si))
    done = short_dft(values, 1, real_out=True)
    for n in range(16):
        emit(n, done[n][0])


def rolled(x, shift):
    return pltpu.roll(x, shift, 1)


def start_copies(pairs, sems):
    copies = [pltpu.make_async_copy(src, dst, sems.at[n]) for n, (src, dst) in enumerate(pairs)]
    for copy in copies:
        copy.start()
    return copies


def columns_kernel(
    plane_hbm, bin_hbm, eff_hbm, dens_hbm, col_hbm, row_hbm, table_hbm, twid_hbm,
    out_ref, row_out, mix_out,
    plane_ref, bin_ref, eff_ref, dens_ref, col_ref, row_ref, table_ref, twid_ref, sems,
):
    pairs = [
        (plane_hbm, plane_ref), (dens_hbm, dens_ref), (col_hbm, col_ref), (twid_hbm, twid_ref),
        (table_hbm, table_ref), (row_hbm, row_ref), (bin_hbm, bin_ref), (eff_hbm, eff_ref),
    ]
    copies = start_copies(pairs, sems)
    for copy in copies[:4]:
        copy.wait()
    plane = plane_ref[lax.axis_index("los")]

    def emit(m, value):
        out_ref[32 * m : 32 * m + 32, :] = value

    def weight(b, s):
        other = plane_ref[s]
        return jnp.where(b >= bin_ref[other], eff_ref[b, other], 0.0)

    def table_of():
        for copy in copies[4:]:
            copy.wait()
        row_out[...] = row_ref[pl.ds(plane, 1), :]
        mix_out[...] = mixing(weight)
        return table_ref[...]

    columns_body(dens_ref[0], col_ref[pl.ds(plane, 1), :], table_of, twid_ref, rolled, emit)


def rows_kernel(got_ref, pos_ref, twid_ref, table2_ref, swap_ref, mixed_ref, table3_ref, out_ref):
    def emit(m, value):
        out_ref[128 * m : 128 * m + 128, :] = value

    def ready():
        return table2_ref[...], table3_ref[...], swap_ref[...]

    rows_body(got_ref[...], pos_ref[...], lax.axis_index("trans"), ready, twid_ref, mixed_ref, rolled, emit)


def final_kernel(got_ref, mix_ref, table_ref, twid_ref, out_ref, wide_ref):
    def emit(n, value):
        for g in range(4):
            jl, comp = g // 2, g % 2
            wide_ref[n, pl.ds(16 * comp + jl, 8, stride=2), :] = value[8 * g : 8 * g + 8]

    def table_of():
        return table_ref[...]

    final_body(
        lambda block: got_ref[128 * block : 128 * block + 128, :], mix_ref[...], table_of, twid_ref, rolled, emit
    )
    for n in range(16):
        for comp in range(2):
            for b in range(4):
                base = 16 * comp + 4 * b
                out_ref[comp, b, :, 128 * n : 128 * n + 128] = wide_ref[n, base : base + 4, :]


def call(kernel, shapes, near, far, scratch=()):
    vmem, hbm = (pl.BlockSpec(memory_space=m) for m in (pltpu.MemorySpace.VMEM, pltpu.MemorySpace.HBM))
    single = len(shapes) == 1
    return pl.pallas_call(
        kernel,
        out_shape=shapes[0] if single else shapes,
        in_specs=[vmem] * len(near) + [hbm] * len(far),
        out_specs=vmem if single else [vmem] * len(shapes),
        scratch_shapes=[pltpu.SMEM(a.shape, a.dtype) if a.size <= 32 else pltpu.VMEM(a.shape, a.dtype) for a in far]
        + [pltpu.SemaphoreType.DMA((len(far),))] * bool(far)
        + list(scratch),
        compiler_params=pltpu.CompilerParams(vmem_limit_bytes=16 << 20),
    )(*near, *[pltpu.with_memory_space_constraint(jnp.asarray(a), pltpu.MemorySpace.HBM) for a in far])


def body(density, row_pos, col_pos, plane_of_slot, plane_bin, efficiency):
    first, second, back, final, swap, plain, mixed = tables()
    sent, row, mix = call(
        columns_kernel,
        [jax.ShapeDtypeStruct((512, 128), BF), jax.ShapeDtypeStruct((1, N), F32), jax.ShapeDtypeStruct((128, 128), BF)],
        [],
        [plane_of_slot, plane_bin, efficiency, density, col_pos, row_pos, pair(first), plain],
    )
    got = lax.all_to_all(sent.reshape(64, 8, 128), "trans", split_axis=0, concat_axis=0, tiled=True)
    sent = call(
        rows_kernel,
        [jax.ShapeDtypeStruct((1024, 128), BF)],
        [got.reshape(512, 128), row, plain, pair(second), swap.astype(BF), mixed, pair(back)],
        [],
    )
    got = lax.all_to_all(sent.reshape(512, 2, 128), ("trans", "los"), split_axis=0, concat_axis=0, tiled=True)
    return call(
        final_kernel,
        [jax.ShapeDtypeStruct((2, 4, 4, N), F32)],
        [got.reshape(1024, 128), mix, pair(final), plain],
        [],
        [pltpu.VMEM((16, 32, 128), F32)],
    )


def solution(mesh):
    placed = (P("los", "trans", None), P(), P(), P(), P(), P())
    return jax.shard_map(
        body,
        mesh=mesh,
        in_specs=placed,
        out_specs=P(None, None, ("trans", "los"), None),
        check_vma=False,
    )
```

```python
import math
import numpy as np
import jax
import jax.numpy as jnp
from jax import lax
from jax.sharding import PartitionSpec as P
from jax.experimental import pallas as pl
from jax.experimental.pallas import tpu as pltpu

BF = jnp.bfloat16
F32 = jnp.float32
N = 2048
HALF = 1024
LEAD = 63


def pair(table):
    table = table.astype(np.float32)
    high = table.astype(BF)
    return np.concatenate([high, (table - high.astype(np.float32)).astype(BF)], axis=0)


def tables():
    n2 = np.arange(128)
    k2p = np.arange(64)
    angle = 2.0 * np.pi * np.outer(n2, k2p) / 128.0
    cos, sin = np.cos(angle).reshape(128, 4, 16), np.sin(angle).reshape(128, 4, 16)
    first = np.concatenate([np.stack([cos, -sin], 2), np.stack([sin, cos], 2)], 0).reshape(256, 128)
    angle = 2.0 * np.pi * np.outer(n2, n2) / 128.0
    cos, sin = np.cos(angle), np.sin(angle)
    second = np.block([[cos, -sin], [sin, cos]])
    order = np.arange(128).reshape(64, 2).T.reshape(-1)
    back = np.block([[cos[:, order], sin[:, order]], [-sin[:, order], cos[:, order]]]) / N
    angle = 2.0 * np.pi * np.outer(k2p, n2) / 128.0
    cos, sin = np.cos(angle).reshape(4, 16, 128), np.sin(angle).reshape(4, 16, 128)
    final = np.concatenate([np.stack([cos, -sin], 1), np.stack([sin, cos], 1)], 3).reshape(128, 256) * (2.0 / N)
    swap = np.zeros((128, 128))
    swap[order, np.arange(128)] = 1.0
    angle = 2.0 * np.pi * np.outer(np.arange(16), n2) / N
    plain = np.concatenate([np.cos(angle), np.sin(angle)], 0).astype(np.float32)
    mixed = np.concatenate([np.cos(angle[:, order]), np.sin(angle[:, order])], 0).astype(np.float32)
    return first, second, back, final, swap, plain, mixed


def add(a, b):
    return b if a is None else a if b is None else a + b


def sub(a, b):
    return a if b is None else -b if a is None else a - b


def turn(value, numer, denom, sign):
    re, im = value
    eighth = (8 * numer // denom) if (8 * numer) % denom == 0 else None
    if eighth == 0:
        return value
    if eighth == 2:
        if sign == 1:
            return (None if im is None else -im, re)
        return (im, -re)
    c, s = math.cos(2 * math.pi * numer / denom), sign * math.sin(2 * math.pi * numer / denom)
    if im is None:
        return (re * c, re * s)
    if re is None:
        return (im * -s, im * c)
    return (re * c - im * s, re * s + im * c)


def short_dft(values, sign):
    n = len(values)
    if n == 1:
        return values
    even = short_dft(values[0::2], sign)
    odd = short_dft(values[1::2], sign)
    low, high = [], []
    for k in range(n // 2):
        t = turn(odd[k], k, n, sign)
        e = even[k]
        low.append((add(e[0], t[0]), add(e[1], t[1])))
        high.append((sub(e[0], t[0]), sub(e[1], t[1])))
    return low + high


def real_dft(values):
    n = len(values)
    if n == 1:
        return [(values[0], None)]
    even, odd = real_dft(values[0::2]), real_dft(values[1::2])
    if n == 2:
        return [(even[0][0] + odd[0][0], None), (even[0][0] - odd[0][0], None)]
    out = [None] * (n // 2 + 1)
    for k in range(n // 4 + 1):
        t, e = turn(odd[k], k, n, -1), even[k]
        out[k] = (add(e[0], t[0]), add(e[1], t[1]))
        if n // 2 - k != k:
            out[n // 2 - k] = (sub(e[0], t[0]), sub(t[1], e[1]) if t[1] is not None else None if e[1] is None else -e[1])
    return out


def real_inverse(values):
    n = 2 * len(values) - 2
    if n == 2:
        return [values[0][0] + values[1][0], values[0][0] - values[1][0]]
    even, odd = [], []
    for k in range(n // 4 + 1):
        x, y = values[k], values[n // 2 - k]
        if n // 2 - k == k:
            even.append((2.0 * x[0], None))
            odd.append((-2.0 * x[1], None))
            continue
        even.append((x[0] + y[0], None if k == 0 else sub(x[1], y[1])))
        if k == 0:
            odd.append((x[0] - y[0], None))
        else:
            odd.append(turn((x[0] - y[0], add(x[1], y[1])), k, n, 1))
    even, odd = real_inverse(even), real_inverse(odd)
    return [v for both in zip(even, odd) for v in both]


def dot(a, b):
    return lax.dot_general(a, b, (((1,), (0,)), ((), ())), preferred_element_type=F32)


def split(x):
    high = x.astype(BF)
    return high, (x - high.astype(F32)).astype(BF)


def dot3(x, table):
    high, low = split(x)
    top = table[: x.shape[1]]
    return dot(jnp.concatenate([high, low, high], axis=1), jnp.concatenate([top, table], axis=0))


def iota(shape, dim):
    return lax.broadcasted_iota(jnp.int32, shape, dim)


def wrapped(p):
    return jnp.where(p >= 1.0 * N, p - 1.0 * N, p)


def block_swap(tiles, roll):
    block = iota((8, 128), 1) // 32
    turned = {(i, d): (roll(tiles[i], 32 * d) if d else tiles[i]) for i in range(4) for d in range(4)}
    out = []
    for q in range(4):
        acc = turned[(0, (0 - q) % 4)]
        for i in range(1, 4):
            acc = jnp.where(block == i, turned[(i, (i - q) % 4)], acc)
        out.append(acc)
    return out


def mixing(plane_of, bin_of, eff):
    col = iota((8, 128), 1)
    slot = (col // 2) % 8
    plane = jnp.zeros((8, 128), jnp.int32)
    for s in range(8):
        plane = jnp.where(slot == s, plane_of(s), plane)
    first_bin = jnp.zeros((8, 128), jnp.int32)
    weight = jnp.zeros((8, 128), F32)
    spread = jnp.concatenate([eff[b : b + 1] for b in range(4) for _ in range(2)], axis=0)
    for p in range(8):
        hit = plane == p
        first_bin = jnp.where(hit, bin_of(p), first_bin)
        weight = jnp.where(hit, spread[:, p : p + 1], weight)
    row = iota((8, 128), 0)
    weight = jnp.where((row // 2 >= first_bin) & (row % 2 == col % 2), weight, 0.0)
    mix = jnp.concatenate([jnp.where(col // 16 == t, weight, 0.0) for t in range(8)], axis=0)
    return jnp.concatenate(split(mix), axis=0)


def columns_body(dens, pos, table_of, twid, roll, emit):
    r, c = iota((32, 32), 0), iota((32, 32), 1)
    perm = jnp.where(c == 4 * (r % 8) + r // 8, 1.0, 0.0).astype(BF)
    dens_f = dot(perm, dens)
    dens_p = dens_f.astype(BF)
    left = jnp.concatenate([dens_p[:, 256 * a : 256 * (a + 1)] for a in range(8)], axis=0)
    lane, row = iota((32, 128), 1), iota((32, 128), 0)
    following = [dens_f[:, (256 * (a + 1)) % N : (256 * (a + 1)) % N + 1] for a in range(8)]
    cell = iota((256, 256), 0).astype(F32).astype(BF)
    zero = jnp.zeros((256, 256), BF)
    tiles = []
    for v in range(8):
        p = wrapped(pos[:, 256 * v : 256 * (v + 1)])
        group = jnp.floor(p * (1.0 / 256.0))
        local = p - 256.0 * group
        base = jnp.floor(local)
        here = (1.0 - (local - base)).astype(BF)
        there = (1.0 - (base + 1.0 - local)).astype(BF)
        table = jnp.where(cell == base.astype(BF), here, jnp.where(cell == (base + 1.0).astype(BF), there, zero))
        edge = jnp.where(base == 255.0, there.astype(F32), 0.0)
        parts = dot(left, table)
        acc, nxt = parts[0:32], jnp.broadcast_to(following[0], (32, 256))
        for a in range(1, 8):
            hit = group == 1.0 * a
            acc = jnp.where(hit, parts[32 * a : 32 * (a + 1)], acc)
            nxt = jnp.where(hit, following[a], nxt)
        acc = acc + edge * nxt
        tiles += [acc[:, :128], acc[:, 128:]]
    freq = real_dft(tiles)
    sign = jnp.where(lane % 2 == 0, 1.0, -1.0)
    nyquist = jnp.sum(freq[0][0] * sign, axis=1, keepdims=True)
    turned = []
    for m in range(16):
        re, im = freq[min(m, 16 - m)]
        co, si = twid[m : m + 1], twid[16 + m : 17 + m]
        if m == 0:
            im = jnp.zeros_like(re)
        elif im is None:
            re, im = re * co, -re * si
        elif m < 8:
            re, im = re * co + im * si, im * co - re * si
        else:
            re, im = re * co - im * si, -(im * co + re * si)
        turned.append(jnp.concatenate([re, im], axis=1))
    result = dot3(jnp.concatenate(turned, axis=0), table_of())
    for m in range(16):
        out = result[32 * m : 32 * m + 32]
        if m == 0:
            base = out[0:1, 0:1].astype(BF).astype(F32)
            out = jnp.where((lane == 0) & (row > 0), out - base, jnp.where(lane == 16, nyquist, out))
        emit(m, jnp.concatenate(block_swap([out[8 * i : 8 * i + 8] for i in range(4)], roll), axis=0).astype(BF))


def rows_body(got, pos, trans, ready, twid, twid_mixed, roll, emit):
    k1p, q = trans // 4, trans % 4
    turned = got.astype(F32).T
    marked = (iota((8, 512), 0) == 0) & (iota((8, 512), 1) % 8 == 0) & (trans == 0)
    base = jnp.where(marked, turned[0:8], 0.0)
    turned = jnp.concatenate([jnp.where(marked, 0.0, turned[0:8]), turned[8:]], axis=0)
    for step in (1, 2, 4):
        base = base + roll(base, step)
    left = jnp.concatenate([turned, roll(turned[0:32], 511), base, roll(base, 511)], axis=0).astype(BF)
    cell = iota((256, 256), 0).astype(F32).astype(BF)
    one, zero = jnp.ones((256, 256), BF), jnp.zeros((256, 256), BF)
    tiles = []
    for u in range(8):
        p = wrapped(pos[:, 256 * u : 256 * (u + 1)])
        group = jnp.floor(p * 0.25)
        local = p - 4.0 * group
        place = group - 8.0 * LEAD
        place = jnp.where(place < 0.0, place + 512.0, place)
        table = jnp.concatenate(
            [jnp.where(cell == place.astype(BF), one, zero), jnp.where(cell == (place - 256.0).astype(BF), one, zero)], axis=0
        )
        parts = dot(left, table)
        acc = total = None
        for s in range(5):
            weight = jnp.maximum(1.0 - jnp.abs(local - 1.0 * s), 0.0).astype(BF).astype(F32)
            acc = add(acc, weight * parts[32 * s : 32 * (s + 1)])
            if s < 4:
                total = add(total, weight)
        extra = total * parts[160:168] + weight * parts[168:176]
        acc = jnp.concatenate([acc[0:8] + extra, acc[8:32]], axis=0)
        tiles += [acc[:, :128], acc[:, 128:]]
    table2, table3, swap = ready()
    first = (iota((16, 128), 0) == 0) & (trans == 0)
    flat = [t[0:8] for t in tiles]
    total = flat[0]
    for t in flat[1:]:
        total = total + t
    mean = jnp.sum(total, axis=1, keepdims=True) * (1.0 / N)
    flat = dot(jnp.concatenate([t - mean for t in flat], axis=0).astype(BF), swap)
    values = []
    for t in tiles:
        re, im = t[0:16], t[16:32]
        values.append((jnp.where(first, im, re), jnp.where(first, 0.0, im)))
    freq = short_dft(values, -1)
    turned = []
    for m in range(16):
        re, im = freq[m]
        if m:
            co, si = twid[m : m + 1], twid[16 + m : 17 + m]
            re, im = re * co + im * si, im * co - re * si
        turned.append(jnp.concatenate([re, im], axis=1))
    spectrum = dot3(jnp.concatenate(turned, axis=0), table2)
    lane = iota((8, 128), 1)
    top = (iota((8, 128), 0) == 0) & (trans == 0)
    w2 = []
    for half in range(2):
        k2 = 256 * q + 16 * (iota((8, 128), 0) + 8 * half) + k1p
        w2.append((jnp.where(top, -HALF, k2) if half == 0 else k2).astype(F32))
    turned = []
    for m in range(16):
        k1 = m + 16 * lane
        w1 = jnp.where(k1 >= HALF, k1 - N, k1).astype(F32)
        square, double = w1 * w1, 2.0 * w1
        rows = [[], [], [], []]
        for half in range(2):
            base = 16 * m + 8 * half
            xr, xi = spectrum[base : base + 8, :128], spectrum[base : base + 8, 128:]
            other = w2[half] * w2[half]
            total = square + other
            inverse = 1.0 / (jnp.maximum(total, 1.0) if m == 0 else total)
            ka = (square - other) * inverse
            kb = double * w2[half] * inverse
            pr, pi = ka * xr, ka * xi
            if m == 0 or half == 0:
                edge = (w1 == -1.0 * HALF) if m == 0 else None
                if half == 0:
                    edge = top if edge is None else edge != top
                odd = jnp.where(edge, kb, 0.0)
                kb = jnp.where(edge, 0.0, kb)
                pr, pi = pr - odd * xi, pi + odd * xr
            for part, value in zip(rows, (pr, pi, kb * xr, kb * xi)):
                part.append(value)
        vr = jnp.concatenate(rows[0] + rows[2], axis=0)
        vi = jnp.concatenate(rows[1] + rows[3], axis=0)
        turned.append(jnp.concatenate([vr, vi], axis=1))
    result = dot3(jnp.concatenate(turned, axis=0), table3)
    back = []
    for m in range(16):
        re, im = result[32 * m : 32 * m + 32, :128], result[32 * m : 32 * m + 32, 128:]
        if m:
            co, si = twid_mixed[m : m + 1], twid_mixed[16 + m : 17 + m]
            re, im = re * co - im * si, im * co + re * si
        back.append((re, im))
    space = short_dft(back, 1)
    low_half = iota((64, 128), 1) < 64
    zero = jnp.zeros((8, 128), F32)
    stacked = []
    for n in range(16):
        re, im = space[n]
        real0 = jnp.concatenate([flat[8 * n : 8 * n + 8], zero], axis=0)
        r0, r1, i0, i1 = re[0:16], re[16:32], im[0:16], im[16:32]
        stacked.append(
            jnp.concatenate(
                [
                    jnp.where(first, real0, r0),
                    jnp.where(first, r0, i0),
                    jnp.where(first, 0.0, r1),
                    jnp.where(first, r1, i1),
                ],
                axis=0,
            )
        )
    for m in range(8):
        a, b = stacked[2 * m], stacked[2 * m + 1]
        top = jnp.where(low_half, a, roll(b, 64))
        bottom = jnp.where(low_half, roll(a, 64), b)
        emit(m, jnp.concatenate([top, bottom], axis=0).astype(BF).T)


def final_body(load, mix, table_of, twid, roll, emit):
    lane = iota((32, 128), 1)
    sign = jnp.where(lane % 2 == 0, 1.0, -1.0)
    lines = []
    for block in range(8):
        summed = dot(mix, load(block))
        summed = summed[0:64] + summed[64:128]
        for half in range(2):
            base = 32 * half
            line = jnp.concatenate(block_swap([summed[base + 8 * i : base + 8 * i + 8] for i in range(4)], roll), axis=0)
            if block == 0 and half == 0:
                nyquist = line[:, 16:17]
                line = jnp.where(lane == 0, 0.5 * line, line)
            lines.append(line)
    result = dot3(jnp.concatenate(lines, axis=0), table_of())
    values = []
    for m in range(16):
        re, im = result[32 * m : 32 * m + 32, :128], result[32 * m : 32 * m + 32, 128:]
        if m == 0:
            values.append((re + (nyquist * (1.0 / N)) * sign, None))
        else:
            co, si = twid[m : m + 1], twid[16 + m : 17 + m]
            values.append((re * co - im * si, im * co + re * si))
    terms = [values[0]]
    for m in range(1, 8):
        x, y = values[m], values[16 - m]
        terms.append((0.5 * (x[0] + y[0]), 0.5 * (x[1] - y[1])))
    terms.append((values[8][0], None))
    done = real_inverse(terms)
    for n in range(16):
        emit(n, done[n])


def rolled(x, shift):
    return pltpu.roll(x, shift, 1)


def start_copies(pairs, sems):
    copies = [pltpu.make_async_copy(src, dst, sems.at[n]) for n, (src, dst) in enumerate(pairs)]
    for copy in copies:
        copy.start()
    return copies


def columns_kernel(
    plane_hbm, bin_hbm, eff_hbm, dens_hbm, col_hbm, row_hbm, table_hbm, twid_hbm,
    out_ref, row_out, mix_out,
    plane_ref, bin_ref, eff_ref, dens_ref, col_ref, row_ref, table_ref, twid_ref, sems,
):
    pairs = [
        (plane_hbm, plane_ref), (dens_hbm, dens_ref), (col_hbm, col_ref), (twid_hbm, twid_ref),
        (table_hbm, table_ref), (row_hbm, row_ref), (bin_hbm, bin_ref), (eff_hbm, eff_ref),
    ]
    copies = start_copies(pairs, sems)
    for copy in copies:
        copy.wait()
    plane = plane_ref[lax.axis_index("los")]

    def emit(m, value):
        for q in range(4):
            place = 8 * ((4 * m + q - LEAD) % 64)
            out_ref[place : place + 8, :] = value[8 * q : 8 * q + 8]

    def table_of():
        row_out[...] = row_ref[pl.ds(plane, 1), :]
        mix_out[...] = mixing(lambda s: plane_ref[s], lambda p: bin_ref[p], eff_ref[...])
        return table_ref[...]

    columns_body(dens_ref[0], col_ref[pl.ds(plane, 1), :], table_of, twid_ref, rolled, emit)


def rows_kernel(got_ref, pos_ref, twid_ref, table2_ref, swap_ref, mixed_ref, table3_ref, out_ref):
    def emit(m, value):
        out_ref[128 * m : 128 * m + 128, :] = value

    def ready():
        return table2_ref[...], table3_ref[...], swap_ref[...]

    rows_body(got_ref[...], pos_ref[...], lax.axis_index("trans"), ready, twid_ref, mixed_ref, rolled, emit)


def final_kernel(got_ref, mix_ref, table_ref, twid_ref, out_ref, wide_ref):
    def emit(n, value):
        for g in range(4):
            jl, comp = g // 2, g % 2
            wide_ref[n, pl.ds(16 * comp + jl, 8, stride=2), :] = value[8 * g : 8 * g + 8]

    def table_of():
        return table_ref[...]

    final_body(
        lambda block: got_ref[128 * block : 128 * block + 128, :], mix_ref[...], table_of, twid_ref, rolled, emit
    )
    for n in range(16):
        for comp in range(2):
            for b in range(4):
                base = 16 * comp + 4 * b
                out_ref[comp, b, :, 128 * n : 128 * n + 128] = wide_ref[n, base : base + 4, :]


def call(kernel, shapes, near, far, scratch=()):
    vmem, hbm = (pl.BlockSpec(memory_space=m) for m in (pltpu.MemorySpace.VMEM, pltpu.MemorySpace.HBM))
    single = len(shapes) == 1
    return pl.pallas_call(
        kernel,
        out_shape=shapes[0] if single else shapes,
        in_specs=[vmem] * len(near) + [hbm] * len(far),
        out_specs=vmem if single else [vmem] * len(shapes),
        scratch_shapes=[pltpu.SMEM(a.shape, a.dtype) if a.ndim == 1 else pltpu.VMEM(a.shape, a.dtype) for a in far]
        + [pltpu.SemaphoreType.DMA((len(far),))] * bool(far)
        + list(scratch),
        compiler_params=pltpu.CompilerParams(vmem_limit_bytes=16 << 20),
    )(*near, *[pltpu.with_memory_space_constraint(jnp.asarray(a), pltpu.MemorySpace.HBM) for a in far])


def body(density, row_pos, col_pos, plane_of_slot, plane_bin, efficiency):
    first, second, back, final, swap, plain, mixed = tables()
    sent, row, mix = call(
        columns_kernel,
        [jax.ShapeDtypeStruct((512, 128), BF), jax.ShapeDtypeStruct((1, N), F32), jax.ShapeDtypeStruct((128, 128), BF)],
        [],
        [plane_of_slot, plane_bin, efficiency, density, col_pos, row_pos, pair(first), plain],
    )
    order = [[(n + LEAD) % 64 for n in range(64)]]
    got = lax.all_to_all(
        sent.reshape(64, 8, 128), "trans", split_axis=0, concat_axis=0, tiled=True, axis_index_groups=order
    )
    sent = call(
        rows_kernel,
        [jax.ShapeDtypeStruct((1024, 128), BF)],
        [got.reshape(512, 128), row, plain, pair(second), swap.astype(BF), mixed, pair(back)],
        [],
    )
    got = lax.all_to_all(sent.reshape(512, 2, 128), ("trans", "los"), split_axis=0, concat_axis=0, tiled=True)
    return call(
        final_kernel,
        [jax.ShapeDtypeStruct((2, 4, 4, N), F32)],
        [got.reshape(1024, 128), mix, pair(final), plain],
        [],
        [pltpu.VMEM((16, 32, 128), F32)],
    )


def solution(mesh):
    placed = (P("los", "trans", None), P(), P(), P(), P(), P())
    return jax.shard_map(
        body,
        mesh=mesh,
        in_specs=placed,
        out_specs=P(None, None, ("trans", "los"), None),
        check_vma=False,
    )
```

```python
import math
import numpy as np
import jax
import jax.numpy as jnp
from jax import lax
from jax.sharding import PartitionSpec as P
from jax.experimental import pallas as pl
from jax.experimental.pallas import tpu as pltpu

BF = jnp.bfloat16
F32 = jnp.float32
N = 2048
HALF = 1024
LEAD = 63


def pair(table):
    table = table.astype(np.float32)
    high = table.astype(BF)
    return np.concatenate([high, (table - high.astype(np.float32)).astype(BF)], axis=0)


def tables():
    n2 = np.arange(128)
    k2p = np.arange(64)
    angle = 2.0 * np.pi * np.outer(n2, k2p) / 128.0
    cos, sin = np.cos(angle).reshape(128, 4, 16), np.sin(angle).reshape(128, 4, 16)
    first = np.concatenate([np.stack([cos, -sin], 2), np.stack([sin, cos], 2)], 0).reshape(256, 128)
    angle = 2.0 * np.pi * np.outer(n2, n2) / 128.0
    cos, sin = np.cos(angle), np.sin(angle)
    second = np.block([[cos, -sin], [sin, cos]])
    order = np.arange(128).reshape(32, 2, 2)[::-1].transpose(2, 0, 1).reshape(-1)
    back = np.block([[cos[:, order], sin[:, order]], [-sin[:, order], cos[:, order]]]) / N
    angle = 2.0 * np.pi * np.outer(k2p, n2) / 128.0
    cos, sin = np.cos(angle).reshape(4, 16, 128), np.sin(angle).reshape(4, 16, 128)
    final = np.concatenate([np.stack([cos, -sin], 1), np.stack([sin, cos], 1)], 3).reshape(128, 256) * (2.0 / N)
    swap = np.zeros((128, 128))
    swap[order, np.arange(128)] = 1.0
    angle = 2.0 * np.pi * np.outer(np.arange(16), n2) / N
    plain = np.concatenate([np.cos(angle), np.sin(angle)], 0).astype(np.float32)
    mixed = np.concatenate([np.cos(angle[:, order]), np.sin(angle[:, order])], 0).astype(np.float32)
    return first, second, back, final, swap, plain, mixed


def add(a, b):
    return b if a is None else a if b is None else a + b


def sub(a, b):
    return a if b is None else -b if a is None else a - b


def turn(value, numer, denom, sign):
    re, im = value
    eighth = (8 * numer // denom) if (8 * numer) % denom == 0 else None
    if eighth == 0:
        return value
    if eighth == 2:
        if sign == 1:
            return (None if im is None else -im, re)
        return (im, -re)
    c, s = math.cos(2 * math.pi * numer / denom), sign * math.sin(2 * math.pi * numer / denom)
    if im is None:
        return (re * c, re * s)
    if re is None:
        return (im * -s, im * c)
    return (re * c - im * s, re * s + im * c)


def short_dft(values, sign):
    n = len(values)
    if n == 1:
        return values
    even = short_dft(values[0::2], sign)
    odd = short_dft(values[1::2], sign)
    low, high = [], []
    for k in range(n // 2):
        t = turn(odd[k], k, n, sign)
        e = even[k]
        low.append((add(e[0], t[0]), add(e[1], t[1])))
        high.append((sub(e[0], t[0]), sub(e[1], t[1])))
    return low + high


def real_dft(values):
    n = len(values)
    if n == 1:
        return [(values[0], None)]
    even, odd = real_dft(values[0::2]), real_dft(values[1::2])
    if n == 2:
        return [(even[0][0] + odd[0][0], None), (even[0][0] - odd[0][0], None)]
    out = [None] * (n // 2 + 1)
    for k in range(n // 4 + 1):
        t, e = turn(odd[k], k, n, -1), even[k]
        out[k] = (add(e[0], t[0]), add(e[1], t[1]))
        if n // 2 - k != k:
            out[n // 2 - k] = (sub(e[0], t[0]), sub(t[1], e[1]) if t[1] is not None else None if e[1] is None else -e[1])
    return out


def real_inverse(values):
    n = 2 * len(values) - 2
    if n == 2:
        return [values[0][0] + values[1][0], values[0][0] - values[1][0]]
    even, odd = [], []
    for k in range(n // 4 + 1):
        x, y = values[k], values[n // 2 - k]
        if n // 2 - k == k:
            even.append((2.0 * x[0], None))
            odd.append((-2.0 * x[1], None))
            continue
        even.append((x[0] + y[0], None if k == 0 else sub(x[1], y[1])))
        if k == 0:
            odd.append((x[0] - y[0], None))
        else:
            odd.append(turn((x[0] - y[0], add(x[1], y[1])), k, n, 1))
    even, odd = real_inverse(even), real_inverse(odd)
    return [v for both in zip(even, odd) for v in both]


def dot(a, b):
    return lax.dot_general(a, b, (((1,), (0,)), ((), ())), preferred_element_type=F32)


def split(x):
    high = x.astype(BF)
    return high, (x - high.astype(F32)).astype(BF)


def dot3(x, table):
    high, low = split(x)
    top = table[: x.shape[1]]
    return dot(jnp.concatenate([high, low, high], axis=1), jnp.concatenate([top, table], axis=0))


def iota(shape, dim):
    return lax.broadcasted_iota(jnp.int32, shape, dim)


def wrapped(p):
    return jnp.where(p >= 1.0 * N, p - 1.0 * N, p)


def block_swap(tiles, roll):
    block = iota((8, 128), 1) // 32
    turned = {(i, d): (roll(tiles[i], 32 * d) if d else tiles[i]) for i in range(4) for d in range(4)}
    out = []
    for q in range(4):
        acc = turned[(0, (0 - q) % 4)]
        for i in range(1, 4):
            acc = jnp.where(block == i, turned[(i, (i - q) % 4)], acc)
        out.append(acc)
    return out


def mixing(plane_of, bin_of, eff):
    col = iota((8, 128), 1)
    slot = 7 - (col // 2) % 8
    plane = jnp.zeros((8, 128), jnp.int32)
    for s in range(8):
        plane = jnp.where(slot == s, plane_of(s), plane)
    first_bin = jnp.zeros((8, 128), jnp.int32)
    weight = jnp.zeros((8, 128), F32)
    spread = jnp.concatenate([eff[b : b + 1] for b in range(4) for _ in range(2)], axis=0)
    for p in range(8):
        hit = plane == p
        first_bin = jnp.where(hit, bin_of(p), first_bin)
        weight = jnp.where(hit, spread[:, p : p + 1], weight)
    row = iota((8, 128), 0)
    weight = jnp.where((row // 2 >= first_bin) & (row % 2 == col % 2), weight, 0.0)
    mix = jnp.concatenate([jnp.where(col // 16 == 7 - t, weight, 0.0) for t in range(8)], axis=0)
    return jnp.concatenate(split(mix), axis=0)


def columns_body(dens, pos, table_of, twid, roll, emit):
    r, c = iota((32, 32), 0), iota((32, 32), 1)
    perm = jnp.where(c == 4 * (r % 8) + r // 8, 1.0, 0.0).astype(BF)
    dens_f = dot(perm, dens)
    dens_p = dens_f.astype(BF)
    left = jnp.concatenate([dens_p[:, 256 * a : 256 * (a + 1)] for a in range(8)], axis=0)
    lane, row = iota((32, 128), 1), iota((32, 128), 0)
    following = [dens_f[:, (256 * (a + 1)) % N : (256 * (a + 1)) % N + 1] for a in range(8)]
    cell = iota((256, 256), 0).astype(F32).astype(BF)
    zero = jnp.zeros((256, 256), BF)
    tiles = []
    for v in range(8):
        p = wrapped(pos[:, 256 * v : 256 * (v + 1)])
        group = jnp.floor(p * (1.0 / 256.0))
        local = p - 256.0 * group
        base = jnp.floor(local)
        here = (1.0 - (local - base)).astype(BF)
        there = (1.0 - (base + 1.0 - local)).astype(BF)
        table = jnp.where(cell == base.astype(BF), here, jnp.where(cell == (base + 1.0).astype(BF), there, zero))
        edge = jnp.where(base == 255.0, there.astype(F32), 0.0)
        parts = dot(left, table)
        acc, nxt = parts[0:32], jnp.broadcast_to(following[0], (32, 256))
        for a in range(1, 8):
            hit = group == 1.0 * a
            acc = jnp.where(hit, parts[32 * a : 32 * (a + 1)], acc)
            nxt = jnp.where(hit, following[a], nxt)
        acc = acc + edge * nxt
        tiles += [acc[:, :128], acc[:, 128:]]
    freq = real_dft(tiles)
    sign = jnp.where(lane % 2 == 0, 1.0, -1.0)
    nyquist = jnp.sum(freq[0][0] * sign, axis=1, keepdims=True)
    turned = []
    for m in range(16):
        re, im = freq[min(m, 16 - m)]
        co, si = twid[m : m + 1], twid[16 + m : 17 + m]
        if m == 0:
            im = jnp.zeros_like(re)
        elif im is None:
            re, im = re * co, -re * si
        elif m < 8:
            re, im = re * co + im * si, im * co - re * si
        else:
            re, im = re * co - im * si, -(im * co + re * si)
        turned.append(jnp.concatenate([re, im], axis=1))
    result = dot3(jnp.concatenate(turned, axis=0), table_of())
    for m in range(16):
        out = result[32 * m : 32 * m + 32]
        if m == 0:
            base = out[0:1, 0:1].astype(BF).astype(F32)
            out = jnp.where((lane == 0) & (row > 0), out - base, jnp.where(lane == 16, nyquist, out))
        emit(m, jnp.concatenate(block_swap([out[8 * i : 8 * i + 8] for i in range(4)], roll), axis=0).astype(BF))


def rows_body(got, pos, trans, ready, twid, twid_mixed, roll, emit):
    k1p, q = trans // 4, trans % 4
    turned = got.astype(F32).T
    marked = (iota((8, 512), 0) == 0) & (iota((8, 512), 1) % 8 == 0) & (trans == 0)
    base = jnp.where(marked, turned[0:8], 0.0)
    turned = jnp.concatenate([jnp.where(marked, 0.0, turned[0:8]), turned[8:]], axis=0)
    for step in (1, 2, 4):
        base = base + roll(base, step)
    left = jnp.concatenate([turned, roll(turned[0:32], 511), base, roll(base, 511)], axis=0).astype(BF)
    cell = iota((256, 256), 0).astype(F32).astype(BF)
    one, zero = jnp.ones((256, 256), BF), jnp.zeros((256, 256), BF)
    tiles = []
    for u in range(8):
        p = wrapped(pos[:, 256 * u : 256 * (u + 1)])
        group = jnp.floor(p * 0.25)
        local = p - 4.0 * group
        place = group - 8.0 * LEAD
        place = jnp.where(place < 0.0, place + 512.0, place)
        table = jnp.concatenate(
            [jnp.where(cell == place.astype(BF), one, zero), jnp.where(cell == (place - 256.0).astype(BF), one, zero)], axis=0
        )
        parts = dot(left, table)
        acc = total = None
        for s in range(5):
            weight = jnp.maximum(1.0 - jnp.abs(local - 1.0 * s), 0.0).astype(BF).astype(F32)
            acc = add(acc, weight * parts[32 * s : 32 * (s + 1)])
            if s < 4:
                total = add(total, weight)
        extra = total * parts[160:168] + weight * parts[168:176]
        acc = jnp.concatenate([acc[0:8] + extra, acc[8:32]], axis=0)
        tiles += [acc[:, :128], acc[:, 128:]]
    table2, table3, swap = ready()
    first = (iota((16, 128), 0) == 0) & (trans == 0)
    flat = [t[0:8] for t in tiles]
    total = flat[0]
    for t in flat[1:]:
        total = total + t
    mean = jnp.sum(total, axis=1, keepdims=True) * (1.0 / N)
    flat = dot(jnp.concatenate([t - mean for t in flat], axis=0).astype(BF), swap)
    values = []
    for t in tiles:
        re, im = t[0:16], t[16:32]
        values.append((jnp.where(first, im, re), jnp.where(first, 0.0, im)))
    freq = short_dft(values, -1)
    turned = []
    for m in range(16):
        re, im = freq[m]
        if m:
            co, si = twid[m : m + 1], twid[16 + m : 17 + m]
            re, im = re * co + im * si, im * co - re * si
        turned.append(jnp.concatenate([re, im], axis=1))
    spectrum = dot3(jnp.concatenate(turned, axis=0), table2)
    lane = iota((8, 128), 1)
    top = (iota((8, 128), 0) == 0) & (trans == 0)
    w2 = []
    for half in range(2):
        k2 = 256 * q + 16 * (iota((8, 128), 0) + 8 * half) + k1p
        w2.append((jnp.where(top, -HALF, k2) if half == 0 else k2).astype(F32))
    turned = []
    for m in range(16):
        k1 = m + 16 * lane
        w1 = jnp.where(k1 >= HALF, k1 - N, k1).astype(F32)
        square, double = w1 * w1, 2.0 * w1
        rows = [[], [], [], []]
        for half in range(2):
            base = 16 * m + 8 * half
            xr, xi = spectrum[base : base + 8, :128], spectrum[base : base + 8, 128:]
            other = w2[half] * w2[half]
            total = square + other
            inverse = 1.0 / (jnp.maximum(total, 1.0) if m == 0 else total)
            ka = (square - other) * inverse
            kb = double * w2[half] * inverse
            pr, pi = ka * xr, ka * xi
            if m == 0 or half == 0:
                edge = (w1 == -1.0 * HALF) if m == 0 else None
                if half == 0:
                    edge = top if edge is None else edge != top
                odd = jnp.where(edge, kb, 0.0)
                kb = jnp.where(edge, 0.0, kb)
                pr, pi = pr - odd * xi, pi + odd * xr
            for part, value in zip(rows, (pr, pi, kb * xr, kb * xi)):
                part.append(value)
        vr = jnp.concatenate(rows[0] + rows[2], axis=0)
        vi = jnp.concatenate(rows[1] + rows[3], axis=0)
        turned.append(jnp.concatenate([vr, vi], axis=1))
    result = dot3(jnp.concatenate(turned, axis=0), table3)
    back = []
    for m in range(16):
        re, im = result[32 * m : 32 * m + 32, :128], result[32 * m : 32 * m + 32, 128:]
        if m:
            co, si = twid_mixed[m : m + 1], twid_mixed[16 + m : 17 + m]
            re, im = re * co - im * si, im * co + re * si
        back.append((re, im))
    space = short_dft(back, 1)
    low_half = iota((64, 128), 1) < 64
    zero = jnp.zeros((8, 128), F32)
    stacked = []
    for n in range(16):
        re, im = space[n]
        real0 = jnp.concatenate([flat[8 * n : 8 * n + 8], zero], axis=0)
        r0, r1, i0, i1 = re[0:16], re[16:32], im[0:16], im[16:32]
        stacked.append(
            jnp.concatenate(
                [
                    jnp.where(first, real0, r0),
                    jnp.where(first, r0, i0),
                    jnp.where(first, 0.0, r1),
                    jnp.where(first, r1, i1),
                ],
                axis=0,
            )
        )
    for m in range(8):
        a, b = stacked[15 - 2 * m], stacked[14 - 2 * m]
        top = jnp.where(low_half, a, roll(b, 64))
        bottom = jnp.where(low_half, roll(a, 64), b)
        emit(m, jnp.concatenate([top, bottom], axis=0).astype(BF).T)


def final_body(load, mix, table_of, twid, roll, emit):
    lane = iota((32, 128), 1)
    sign = jnp.where(lane % 2 == 0, 1.0, -1.0)
    lines = []
    for block in range(8):
        summed = dot(mix, load(block))
        summed = summed[0:64] + summed[64:128]
        for half in range(2):
            base = 32 * half
            line = jnp.concatenate(block_swap([summed[base + 8 * i : base + 8 * i + 8] for i in range(4)], roll), axis=0)
            if block == 0 and half == 0:
                nyquist = line[:, 16:17]
                line = jnp.where(lane == 0, 0.5 * line, line)
            lines.append(line)
    result = dot3(jnp.concatenate(lines, axis=0), table_of())
    values = []
    for m in range(16):
        re, im = result[32 * m : 32 * m + 32, :128], result[32 * m : 32 * m + 32, 128:]
        if m == 0:
            values.append((re + (nyquist * (1.0 / N)) * sign, None))
        else:
            co, si = twid[m : m + 1], twid[16 + m : 17 + m]
            values.append((re * co - im * si, im * co + re * si))
    terms = [values[0]]
    for m in range(1, 8):
        x, y = values[m], values[16 - m]
        terms.append((0.5 * (x[0] + y[0]), 0.5 * (x[1] - y[1])))
    terms.append((values[8][0], None))
    done = real_inverse(terms)
    for n in range(16):
        emit(n, done[n])


def rolled(x, shift):
    return pltpu.roll(x, shift, 1)


def start_copies(pairs, sems):
    copies = [pltpu.make_async_copy(src, dst, sems.at[n]) for n, (src, dst) in enumerate(pairs)]
    for copy in copies:
        copy.start()
    return copies


def columns_kernel(
    plane_hbm, bin_hbm, eff_hbm, dens_hbm, col_hbm, row_hbm, table_hbm, twid_hbm,
    out_ref, row_out, mix_out,
    plane_ref, bin_ref, eff_ref, dens_ref, col_ref, row_ref, table_ref, twid_ref, sems,
):
    pairs = [
        (plane_hbm, plane_ref), (dens_hbm, dens_ref), (col_hbm, col_ref), (twid_hbm, twid_ref),
        (table_hbm, table_ref), (row_hbm, row_ref), (bin_hbm, bin_ref), (eff_hbm, eff_ref),
    ]
    copies = start_copies(pairs, sems)
    for copy in copies:
        copy.wait()
    plane = plane_ref[lax.axis_index("los")]

    def emit(m, value):
        for q in range(4):
            place = 8 * ((4 * m + q - LEAD) % 64)
            out_ref[place : place + 8, :] = value[8 * q : 8 * q + 8]

    def table_of():
        row_out[...] = row_ref[pl.ds(plane, 1), :]
        mix_out[...] = mixing(lambda s: plane_ref[s], lambda p: bin_ref[p], eff_ref[...])
        return table_ref[...]

    columns_body(dens_ref[0], col_ref[pl.ds(plane, 1), :], table_of, twid_ref, rolled, emit)


def rows_kernel(got_ref, pos_ref, twid_ref, table2_ref, swap_ref, mixed_ref, table3_ref, out_ref):
    def emit(m, value):
        out_ref[128 * m : 128 * m + 128, :] = value

    def ready():
        return table2_ref[...], table3_ref[...], swap_ref[...]

    rows_body(got_ref[...], pos_ref[...], lax.axis_index("trans"), ready, twid_ref, mixed_ref, rolled, emit)


def final_kernel(got_ref, mix_ref, table_ref, twid_ref, out_ref, wide_ref):
    def emit(n, value):
        for g in range(4):
            jl, comp = g // 2, g % 2
            wide_ref[n, pl.ds(16 * comp + jl, 8, stride=2), :] = value[8 * g : 8 * g + 8]

    def table_of():
        return table_ref[...]

    final_body(
        lambda block: got_ref[128 * (7 - block) : 128 * (7 - block) + 128, :], mix_ref[...], table_of, twid_ref, rolled, emit
    )
    for n in range(16):
        for comp in range(2):
            for b in range(4):
                base = 16 * comp + 4 * b
                out_ref[comp, b, :, 128 * n : 128 * n + 128] = wide_ref[n, base : base + 4, :]


def call(kernel, shapes, near, far, scratch=()):
    vmem, hbm = (pl.BlockSpec(memory_space=m) for m in (pltpu.MemorySpace.VMEM, pltpu.MemorySpace.HBM))
    single = len(shapes) == 1
    return pl.pallas_call(
        kernel,
        out_shape=shapes[0] if single else shapes,
        in_specs=[vmem] * len(near) + [hbm] * len(far),
        out_specs=vmem if single else [vmem] * len(shapes),
        scratch_shapes=[pltpu.SMEM(a.shape, a.dtype) if a.ndim == 1 else pltpu.VMEM(a.shape, a.dtype) for a in far]
        + [pltpu.SemaphoreType.DMA((len(far),))] * bool(far)
        + list(scratch),
        compiler_params=pltpu.CompilerParams(vmem_limit_bytes=16 << 20),
    )(*near, *[pltpu.with_memory_space_constraint(jnp.asarray(a), pltpu.MemorySpace.HBM) for a in far])


def body(density, row_pos, col_pos, plane_of_slot, plane_bin, efficiency):
    first, second, back, final, swap, plain, mixed = tables()
    sent, row, mix = call(
        columns_kernel,
        [jax.ShapeDtypeStruct((512, 128), BF), jax.ShapeDtypeStruct((1, N), F32), jax.ShapeDtypeStruct((128, 128), BF)],
        [],
        [plane_of_slot, plane_bin, efficiency, density, col_pos, row_pos, pair(first), plain],
    )
    order = [[(n + LEAD) % 64 for n in range(64)]]
    got = lax.all_to_all(
        sent.reshape(64, 8, 128), "trans", split_axis=0, concat_axis=0, tiled=True, axis_index_groups=order
    )
    sent = call(
        rows_kernel,
        [jax.ShapeDtypeStruct((1024, 128), BF)],
        [got.reshape(512, 128), row, plain, pair(second), swap.astype(BF), mixed, pair(back)],
        [],
    )
    order = [list(range(511, -1, -1))]
    got = lax.all_to_all(
        sent.reshape(512, 2, 128), ("trans", "los"), split_axis=0, concat_axis=0, tiled=True, axis_index_groups=order
    )
    return call(
        final_kernel,
        [jax.ShapeDtypeStruct((2, 4, 4, N), F32)],
        [got.reshape(1024, 128), mix, pair(final), plain],
        [],
        [pltpu.VMEM((16, 32, 128), F32)],
    )


def solution(mesh):
    placed = (P("los", "trans", None), P(), P(), P(), P(), P())
    return jax.shard_map(
        body,
        mesh=mesh,
        in_specs=placed,
        out_specs=P(None, None, ("trans", "los"), None),
        check_vma=False,
    )
```

```python
import math
import numpy as np
import jax
import jax.numpy as jnp
from jax import lax
from jax.sharding import PartitionSpec as P
from jax.experimental import pallas as pl
from jax.experimental.pallas import tpu as pltpu

BF = jnp.bfloat16
F32 = jnp.float32
N = 2048
HALF = 1024
LEAD = 63


def pair(table):
    table = table.astype(np.float32)
    high = table.astype(BF)
    return np.concatenate([high, (table - high.astype(np.float32)).astype(BF)], axis=0)


def tables():
    n2 = np.arange(128)
    k2p = np.arange(64)
    angle = 2.0 * np.pi * np.outer(n2, k2p) / 128.0
    cos, sin = np.cos(angle).reshape(128, 4, 16), np.sin(angle).reshape(128, 4, 16)
    first = np.concatenate([np.stack([cos, -sin], 2), np.stack([sin, cos], 2)], 0).reshape(256, 128)
    angle = 2.0 * np.pi * np.outer(n2, n2) / 128.0
    cos, sin = np.cos(angle), np.sin(angle)
    second = np.block([[cos, -sin], [sin, cos]])
    order = np.arange(128).reshape(16, 2, 2, 2)[::-1].transpose(3, 1, 0, 2).reshape(-1)
    back = np.block([[cos[:, order], sin[:, order]], [-sin[:, order], cos[:, order]]]) / N
    angle = 2.0 * np.pi * np.outer(k2p, n2) / 128.0
    cos, sin = np.cos(angle).reshape(4, 16, 128), np.sin(angle).reshape(4, 16, 128)
    final = np.concatenate([np.stack([cos, -sin], 1), np.stack([sin, cos], 1)], 3).reshape(128, 256) * (2.0 / N)
    swap = np.zeros((128, 128))
    swap[order, np.arange(128)] = 1.0
    angle = 2.0 * np.pi * np.outer(np.arange(16), n2) / N
    plain = np.concatenate([np.cos(angle), np.sin(angle)], 0).astype(np.float32)
    mixed = np.concatenate([np.cos(angle[:, order]), np.sin(angle[:, order])], 0).astype(np.float32)
    return first, second, back, final, swap, plain, mixed


def add(a, b):
    return b if a is None else a if b is None else a + b


def sub(a, b):
    return a if b is None else -b if a is None else a - b


def turn(value, numer, denom, sign):
    re, im = value
    eighth = (8 * numer // denom) if (8 * numer) % denom == 0 else None
    if eighth == 0:
        return value
    if eighth == 2:
        if sign == 1:
            return (None if im is None else -im, re)
        return (im, -re)
    c, s = math.cos(2 * math.pi * numer / denom), sign * math.sin(2 * math.pi * numer / denom)
    if im is None:
        return (re * c, re * s)
    if re is None:
        return (im * -s, im * c)
    return (re * c - im * s, re * s + im * c)


def short_dft(values, sign):
    n = len(values)
    if n == 1:
        return values
    even = short_dft(values[0::2], sign)
    odd = short_dft(values[1::2], sign)
    low, high = [], []
    for k in range(n // 2):
        t = turn(odd[k], k, n, sign)
        e = even[k]
        low.append((add(e[0], t[0]), add(e[1], t[1])))
        high.append((sub(e[0], t[0]), sub(e[1], t[1])))
    return low + high


def real_dft(values):
    n = len(values)
    if n == 1:
        return [(values[0], None)]
    even, odd = real_dft(values[0::2]), real_dft(values[1::2])
    if n == 2:
        return [(even[0][0] + odd[0][0], None), (even[0][0] - odd[0][0], None)]
    out = [None] * (n // 2 + 1)
    for k in range(n // 4 + 1):
        t, e = turn(odd[k], k, n, -1), even[k]
        out[k] = (add(e[0], t[0]), add(e[1], t[1]))
        if n // 2 - k != k:
            out[n // 2 - k] = (sub(e[0], t[0]), sub(t[1], e[1]) if t[1] is not None else None if e[1] is None else -e[1])
    return out


def real_inverse(values):
    n = 2 * len(values) - 2
    if n == 2:
        return [values[0][0] + values[1][0], values[0][0] - values[1][0]]
    even, odd = [], []
    for k in range(n // 4 + 1):
        x, y = values[k], values[n // 2 - k]
        if n // 2 - k == k:
            even.append((2.0 * x[0], None))
            odd.append((-2.0 * x[1], None))
            continue
        even.append((x[0] + y[0], None if k == 0 else sub(x[1], y[1])))
        if k == 0:
            odd.append((x[0] - y[0], None))
        else:
            odd.append(turn((x[0] - y[0], add(x[1], y[1])), k, n, 1))
    even, odd = real_inverse(even), real_inverse(odd)
    return [v for both in zip(even, odd) for v in both]


def dot(a, b):
    return lax.dot_general(a, b, (((1,), (0,)), ((), ())), preferred_element_type=F32)


def split(x):
    high = x.astype(BF)
    return high, (x - high.astype(F32)).astype(BF)


def dot3(x, table):
    high, low = split(x)
    top = table[: x.shape[1]]
    return dot(jnp.concatenate([high, low, high], axis=1), jnp.concatenate([top, table], axis=0))


def iota(shape, dim):
    return lax.broadcasted_iota(jnp.int32, shape, dim)


def wrapped(p):
    return jnp.where(p >= 1.0 * N, p - 1.0 * N, p)


def block_swap(tiles, roll):
    block = iota((8, 128), 1) // 32
    turned = {(i, d): (roll(tiles[i], 32 * d) if d else tiles[i]) for i in range(4) for d in range(4)}
    out = []
    for q in range(4):
        acc = turned[(0, (0 - q) % 4)]
        for i in range(1, 4):
            acc = jnp.where(block == i, turned[(i, (i - q) % 4)], acc)
        out.append(acc)
    return out


def mixing(core, plane_of, bin_of, eff):
    col = iota((8, 128), 1)
    place = (col // 2) % 8
    slot = 2 * (3 - place // 2) + jnp.where(core == 0, place % 2, 1 - place % 2)
    plane = jnp.zeros((8, 128), jnp.int32)
    for s in range(8):
        plane = jnp.where(slot == s, plane_of(s), plane)
    first_bin = jnp.zeros((8, 128), jnp.int32)
    weight = jnp.zeros((8, 128), F32)
    spread = jnp.concatenate([eff[b : b + 1] for b in range(4) for _ in range(2)], axis=0)
    for p in range(8):
        hit = plane == p
        first_bin = jnp.where(hit, bin_of(p), first_bin)
        weight = jnp.where(hit, spread[:, p : p + 1], weight)
    row = iota((8, 128), 0)
    weight = jnp.where((row // 2 >= first_bin) & (row % 2 == col % 2), weight, 0.0)
    mix = jnp.concatenate([jnp.where(col // 16 == 7 - t, weight, 0.0) for t in range(8)], axis=0)
    return jnp.concatenate(split(mix), axis=0)


def columns_body(dens, pos, table_of, twid, roll, emit):
    r, c = iota((32, 32), 0), iota((32, 32), 1)
    perm = jnp.where(c == 4 * (r % 8) + r // 8, 1.0, 0.0).astype(BF)
    dens_f = dot(perm, dens)
    dens_p = dens_f.astype(BF)
    left = jnp.concatenate([dens_p[:, 256 * a : 256 * (a + 1)] for a in range(8)], axis=0)
    lane, row = iota((32, 128), 1), iota((32, 128), 0)
    following = [dens_f[:, (256 * (a + 1)) % N : (256 * (a + 1)) % N + 1] for a in range(8)]
    cell = iota((256, 256), 0).astype(F32).astype(BF)
    zero = jnp.zeros((256, 256), BF)
    tiles = []
    for v in range(8):
        p = wrapped(pos[:, 256 * v : 256 * (v + 1)])
        group = jnp.floor(p * (1.0 / 256.0))
        local = p - 256.0 * group
        base = jnp.floor(local)
        here = (1.0 - (local - base)).astype(BF)
        there = (1.0 - (base + 1.0 - local)).astype(BF)
        table = jnp.where(cell == base.astype(BF), here, jnp.where(cell == (base + 1.0).astype(BF), there, zero))
        edge = jnp.where(base == 255.0, there.astype(F32), 0.0)
        parts = dot(left, table)
        acc, nxt = parts[0:32], jnp.broadcast_to(following[0], (32, 256))
        for a in range(1, 8):
            hit = group == 1.0 * a
            acc = jnp.where(hit, parts[32 * a : 32 * (a + 1)], acc)
            nxt = jnp.where(hit, following[a], nxt)
        acc = acc + edge * nxt
        tiles += [acc[:, :128], acc[:, 128:]]
    freq = real_dft(tiles)
    sign = jnp.where(lane % 2 == 0, 1.0, -1.0)
    nyquist = jnp.sum(freq[0][0] * sign, axis=1, keepdims=True)
    turned = []
    for m in range(16):
        re, im = freq[min(m, 16 - m)]
        co, si = twid[m : m + 1], twid[16 + m : 17 + m]
        if m == 0:
            im = jnp.zeros_like(re)
        elif im is None:
            re, im = re * co, -re * si
        elif m < 8:
            re, im = re * co + im * si, im * co - re * si
        else:
            re, im = re * co - im * si, -(im * co + re * si)
        turned.append(jnp.concatenate([re, im], axis=1))
    result = dot3(jnp.concatenate(turned, axis=0), table_of())
    for m in range(16):
        out = result[32 * m : 32 * m + 32]
        if m == 0:
            base = out[0:1, 0:1].astype(BF).astype(F32)
            out = jnp.where((lane == 0) & (row > 0), out - base, jnp.where(lane == 16, nyquist, out))
        emit(m, jnp.concatenate(block_swap([out[8 * i : 8 * i + 8] for i in range(4)], roll), axis=0).astype(BF))


def rows_body(got, pos, trans, ready, twid, twid_mixed, roll, emit):
    k1p, q = trans // 4, trans % 4
    turned = got.astype(F32).T
    marked = (iota((8, 512), 0) == 0) & (iota((8, 512), 1) % 8 == 0) & (trans == 0)
    base = jnp.where(marked, turned[0:8], 0.0)
    turned = jnp.concatenate([jnp.where(marked, 0.0, turned[0:8]), turned[8:]], axis=0)
    for step in (1, 2, 4):
        base = base + roll(base, step)
    left = jnp.concatenate([turned, roll(turned[0:32], 511), base, roll(base, 511)], axis=0).astype(BF)
    cell = iota((256, 256), 0).astype(F32).astype(BF)
    one, zero = jnp.ones((256, 256), BF), jnp.zeros((256, 256), BF)
    tiles = []
    for u in range(8):
        p = wrapped(pos[:, 256 * u : 256 * (u + 1)])
        group = jnp.floor(p * 0.25)
        local = p - 4.0 * group
        place = group - 8.0 * LEAD
        place = jnp.where(place < 0.0, place + 512.0, place)
        table = jnp.concatenate(
            [jnp.where(cell == place.astype(BF), one, zero), jnp.where(cell == (place - 256.0).astype(BF), one, zero)], axis=0
        )
        parts = dot(left, table)
        acc = total = None
        for s in range(5):
            weight = jnp.maximum(1.0 - jnp.abs(local - 1.0 * s), 0.0).astype(BF).astype(F32)
            acc = add(acc, weight * parts[32 * s : 32 * (s + 1)])
            if s < 4:
                total = add(total, weight)
        extra = total * parts[160:168] + weight * parts[168:176]
        acc = jnp.concatenate([acc[0:8] + extra, acc[8:32]], axis=0)
        tiles += [acc[:, :128], acc[:, 128:]]
    table2, table3, swap = ready()
    first = (iota((16, 128), 0) == 0) & (trans == 0)
    flat = [t[0:8] for t in tiles]
    total = flat[0]
    for t in flat[1:]:
        total = total + t
    mean = jnp.sum(total, axis=1, keepdims=True) * (1.0 / N)
    flat = dot(jnp.concatenate([t - mean for t in flat], axis=0).astype(BF), swap)
    values = []
    for t in tiles:
        re, im = t[0:16], t[16:32]
        values.append((jnp.where(first, im, re), jnp.where(first, 0.0, im)))
    freq = short_dft(values, -1)
    turned = []
    for m in range(16):
        re, im = freq[m]
        if m:
            co, si = twid[m : m + 1], twid[16 + m : 17 + m]
            re, im = re * co + im * si, im * co - re * si
        turned.append(jnp.concatenate([re, im], axis=1))
    spectrum = dot3(jnp.concatenate(turned, axis=0), table2)
    lane = iota((8, 128), 1)
    top = (iota((8, 128), 0) == 0) & (trans == 0)
    w2 = []
    for half in range(2):
        k2 = 256 * q + 16 * (iota((8, 128), 0) + 8 * half) + k1p
        w2.append((jnp.where(top, -HALF, k2) if half == 0 else k2).astype(F32))
    turned = []
    for m in range(16):
        k1 = m + 16 * lane
        w1 = jnp.where(k1 >= HALF, k1 - N, k1).astype(F32)
        square, double = w1 * w1, 2.0 * w1
        rows = [[], [], [], []]
        for half in range(2):
            base = 16 * m + 8 * half
            xr, xi = spectrum[base : base + 8, :128], spectrum[base : base + 8, 128:]
            other = w2[half] * w2[half]
            total = square + other
            inverse = 1.0 / (jnp.maximum(total, 1.0) if m == 0 else total)
            ka = (square - other) * inverse
            kb = double * w2[half] * inverse
            pr, pi = ka * xr, ka * xi
            if m == 0 or half == 0:
                edge = (w1 == -1.0 * HALF) if m == 0 else None
                if half == 0:
                    edge = top if edge is None else edge != top
                odd = jnp.where(edge, kb, 0.0)
                kb = jnp.where(edge, 0.0, kb)
                pr, pi = pr - odd * xi, pi + odd * xr
            for part, value in zip(rows, (pr, pi, kb * xr, kb * xi)):
                part.append(value)
        vr = jnp.concatenate(rows[0] + rows[2], axis=0)
        vi = jnp.concatenate(rows[1] + rows[3], axis=0)
        turned.append(jnp.concatenate([vr, vi], axis=1))
    result = dot3(jnp.concatenate(turned, axis=0), table3)
    back = []
    for m in range(16):
        re, im = result[32 * m : 32 * m + 32, :128], result[32 * m : 32 * m + 32, 128:]
        if m:
            co, si = twid_mixed[m : m + 1], twid_mixed[16 + m : 17 + m]
            re, im = re * co - im * si, im * co + re * si
        back.append((re, im))
    space = short_dft(back, 1)
    low_half = iota((64, 128), 1) < 64
    zero = jnp.zeros((8, 128), F32)
    stacked = []
    for n in range(16):
        re, im = space[n]
        real0 = jnp.concatenate([flat[8 * n : 8 * n + 8], zero], axis=0)
        r0, r1, i0, i1 = re[0:16], re[16:32], im[0:16], im[16:32]
        stacked.append(
            jnp.concatenate(
                [
                    jnp.where(first, real0, r0),
                    jnp.where(first, r0, i0),
                    jnp.where(first, 0.0, r1),
                    jnp.where(first, r1, i1),
                ],
                axis=0,
            )
        )
    for m in range(8):
        a, b = stacked[15 - 2 * m], stacked[14 - 2 * m]
        top = jnp.where(low_half, a, roll(b, 64))
        bottom = jnp.where(low_half, roll(a, 64), b)
        emit(m, jnp.concatenate([top, bottom], axis=0).astype(BF).T)


def final_body(load, mix, table_of, twid, roll, emit):
    lane = iota((32, 128), 1)
    sign = jnp.where(lane % 2 == 0, 1.0, -1.0)
    lines = []
    for block in range(8):
        summed = dot(mix, load(block))
        summed = summed[0:64] + summed[64:128]
        for half in range(2):
            base = 32 * half
            line = jnp.concatenate(block_swap([summed[base + 8 * i : base + 8 * i + 8] for i in range(4)], roll), axis=0)
            if block == 0 and half == 0:
                nyquist = line[:, 16:17]
                line = jnp.where(lane == 0, 0.5 * line, line)
            lines.append(line)
    result = dot3(jnp.concatenate(lines, axis=0), table_of())
    values = []
    for m in range(16):
        re, im = result[32 * m : 32 * m + 32, :128], result[32 * m : 32 * m + 32, 128:]
        if m == 0:
            values.append((re + (nyquist * (1.0 / N)) * sign, None))
        else:
            co, si = twid[m : m + 1], twid[16 + m : 17 + m]
            values.append((re * co - im * si, im * co + re * si))
    terms = [values[0]]
    for m in range(1, 8):
        x, y = values[m], values[16 - m]
        terms.append((0.5 * (x[0] + y[0]), 0.5 * (x[1] - y[1])))
    terms.append((values[8][0], None))
    done = real_inverse(terms)
    for n in range(16):
        emit(n, done[n])


def rolled(x, shift):
    return pltpu.roll(x, shift, 1)


def start_copies(pairs, sems):
    copies = [pltpu.make_async_copy(src, dst, sems.at[n]) for n, (src, dst) in enumerate(pairs)]
    for copy in copies:
        copy.start()
    return copies


def columns_kernel(
    plane_hbm, bin_hbm, eff_hbm, dens_hbm, col_hbm, row_hbm, table_hbm, twid_hbm,
    out_ref, row_out, mix_out,
    plane_ref, bin_ref, eff_ref, dens_ref, col_ref, row_ref, table_ref, twid_ref, sems,
):
    pairs = [
        (plane_hbm, plane_ref), (dens_hbm, dens_ref), (col_hbm, col_ref), (twid_hbm, twid_ref),
        (table_hbm, table_ref), (row_hbm, row_ref), (bin_hbm, bin_ref), (eff_hbm, eff_ref),
    ]
    copies = start_copies(pairs, sems)
    for copy in copies:
        copy.wait()
    plane = plane_ref[lax.axis_index("los")]

    def emit(m, value):
        for q in range(4):
            place = 8 * ((4 * m + q - LEAD) % 64)
            out_ref[place : place + 8, :] = value[8 * q : 8 * q + 8]

    def table_of():
        row_out[...] = row_ref[pl.ds(plane, 1), :]
        mix_out[...] = mixing(lax.axis_index("los") % 2, lambda s: plane_ref[s], lambda p: bin_ref[p], eff_ref[...])
        return table_ref[...]

    columns_body(dens_ref[0], col_ref[pl.ds(plane, 1), :], table_of, twid_ref, rolled, emit)


def rows_kernel(got_ref, pos_ref, twid_ref, table2_ref, swap_ref, mixed_ref, table3_ref, same_ref, other_ref):
    north = lax.axis_index("los") % 2 == 1

    def emit(m, value):
        zero = jnp.concatenate([value[0:32], value[64:96]], axis=0)
        one = jnp.concatenate([value[32:64], value[96:128]], axis=0)
        same_ref[64 * m : 64 * m + 64, :] = jnp.where(north, one, zero)
        other_ref[64 * m : 64 * m + 64, :] = jnp.where(north, zero, one)

    def ready():
        return table2_ref[...], table3_ref[...], swap_ref[...]

    rows_body(got_ref[...], pos_ref[...], lax.axis_index("trans"), ready, twid_ref, mixed_ref, rolled, emit)


def final_kernel(got_ref, mix_ref, table_ref, twid_ref, out_ref, wide_ref):
    def emit(n, value):
        for g in range(4):
            jl, comp = g // 2, g % 2
            wide_ref[n, pl.ds(16 * comp + jl, 8, stride=2), :] = value[8 * g : 8 * g + 8]

    def table_of():
        return table_ref[...]

    final_body(
        lambda block: got_ref[128 * (7 - block) : 128 * (7 - block) + 128, :], mix_ref[...], table_of, twid_ref, rolled, emit
    )
    for n in range(16):
        for comp in range(2):
            for b in range(4):
                base = 16 * comp + 4 * b
                out_ref[comp, b, :, 128 * n : 128 * n + 128] = wide_ref[n, base : base + 4, :]


def call(kernel, shapes, near, far, scratch=()):
    vmem, hbm = (pl.BlockSpec(memory_space=m) for m in (pltpu.MemorySpace.VMEM, pltpu.MemorySpace.HBM))
    single = len(shapes) == 1
    return pl.pallas_call(
        kernel,
        out_shape=shapes[0] if single else shapes,
        in_specs=[vmem] * len(near) + [hbm] * len(far),
        out_specs=vmem if single else [vmem] * len(shapes),
        scratch_shapes=[pltpu.SMEM(a.shape, a.dtype) if a.ndim == 1 else pltpu.VMEM(a.shape, a.dtype) for a in far]
        + [pltpu.SemaphoreType.DMA((len(far),))] * bool(far)
        + list(scratch),
        compiler_params=pltpu.CompilerParams(vmem_limit_bytes=16 << 20),
    )(*near, *[pltpu.with_memory_space_constraint(jnp.asarray(a), pltpu.MemorySpace.HBM) for a in far])


def body(density, row_pos, col_pos, plane_of_slot, plane_bin, efficiency):
    first, second, back, final, swap, plain, mixed = tables()
    sent, row, mix = call(
        columns_kernel,
        [jax.ShapeDtypeStruct((512, 128), BF), jax.ShapeDtypeStruct((1, N), F32), jax.ShapeDtypeStruct((128, 128), BF)],
        [],
        [plane_of_slot, plane_bin, efficiency, density, col_pos, row_pos, pair(first), plain],
    )
    order = [[(n + LEAD) % 64 for n in range(64)]]
    got = lax.all_to_all(
        sent.reshape(64, 8, 128), "trans", split_axis=0, concat_axis=0, tiled=True, axis_index_groups=order
    )
    same, other = call(
        rows_kernel,
        [jax.ShapeDtypeStruct((512, 128), BF)] * 2,
        [got.reshape(512, 128), row, plain, pair(second), swap.astype(BF), mixed, pair(back)],
        [],
    )
    axes = ("trans", "los")
    other = lax.ppermute(other.reshape(256, 2, 128), axes, [(n, n ^ 1) for n in range(512)])
    sent = jnp.concatenate([same.reshape(256, 2, 128), other], axis=1)
    order = [[2 * n + core for n in range(255, -1, -1)] for core in range(2)]
    got = lax.all_to_all(sent, axes, split_axis=0, concat_axis=0, tiled=True, axis_index_groups=order)
    return call(
        final_kernel,
        [jax.ShapeDtypeStruct((2, 4, 4, N), F32)],
        [got.reshape(1024, 128), mix, pair(final), plain],
        [],
        [pltpu.VMEM((16, 32, 128), F32)],
    )


def solution(mesh):
    placed = (P("los", "trans", None), P(), P(), P(), P(), P())
    return jax.shard_map(
        body,
        mesh=mesh,
        in_specs=placed,
        out_specs=P(None, None, ("trans", "los"), None),
        check_vma=False,
    )
```

```python
import math
import numpy as np
import jax
import jax.numpy as jnp
from jax import lax
from jax.sharding import PartitionSpec as P
from jax.experimental import pallas as pl
from jax.experimental.pallas import tpu as pltpu

BF = jnp.bfloat16
F32 = jnp.float32
N = 2048
HALF = 1024
LEAD = 63
TOP = 7


def pair(table):
    table = table.astype(np.float32)
    high = table.astype(BF)
    return np.concatenate([high, (table - high.astype(np.float32)).astype(BF)], axis=0)


def tables():
    n2 = np.arange(128)
    k2p = np.arange(64)
    angle = 2.0 * np.pi * np.outer(n2, k2p) / 128.0
    cos, sin = np.cos(angle).reshape(128, 4, 16), np.sin(angle).reshape(128, 4, 16)
    first = np.concatenate([np.stack([cos, -sin], 2), np.stack([sin, cos], 2)], 0).reshape(256, 128)
    angle = 2.0 * np.pi * np.outer(n2, n2) / 128.0
    cos, sin = np.cos(angle), np.sin(angle)
    second = np.block([[cos, -sin], [sin, cos]])
    order = np.arange(128).reshape(4, 4, 2, 2, 2)[::-1].transpose(4, 2, 0, 1, 3).reshape(-1)
    back = np.block([[cos[:, order], sin[:, order]], [-sin[:, order], cos[:, order]]]) / N
    angle = 2.0 * np.pi * np.outer(k2p, n2) / 128.0
    cos, sin = np.cos(angle).reshape(4, 16, 128), np.sin(angle).reshape(4, 16, 128)
    final = np.concatenate([np.stack([cos, -sin], 1), np.stack([sin, cos], 1)], 3).reshape(128, 256) * (2.0 / N)
    swap = np.zeros((128, 128))
    swap[order, np.arange(128)] = 1.0
    angle = 2.0 * np.pi * np.outer(np.arange(16), n2) / N
    plain = np.concatenate([np.cos(angle), np.sin(angle)], 0).astype(np.float32)
    mixed = np.concatenate([np.cos(angle[:, order]), np.sin(angle[:, order])], 0).astype(np.float32)
    return first, second, back, final, swap, plain, mixed


def add(a, b):
    return b if a is None else a if b is None else a + b


def sub(a, b):
    return a if b is None else -b if a is None else a - b


def turn(value, numer, denom, sign):
    re, im = value
    eighth = (8 * numer // denom) if (8 * numer) % denom == 0 else None
    if eighth == 0:
        return value
    if eighth == 2:
        if sign == 1:
            return (None if im is None else -im, re)
        return (im, -re)
    c, s = math.cos(2 * math.pi * numer / denom), sign * math.sin(2 * math.pi * numer / denom)
    if im is None:
        return (re * c, re * s)
    if re is None:
        return (im * -s, im * c)
    return (re * c - im * s, re * s + im * c)


def short_dft(values, sign):
    n = len(values)
    if n == 1:
        return values
    even = short_dft(values[0::2], sign)
    odd = short_dft(values[1::2], sign)
    low, high = [], []
    for k in range(n // 2):
        t = turn(odd[k], k, n, sign)
        e = even[k]
        low.append((add(e[0], t[0]), add(e[1], t[1])))
        high.append((sub(e[0], t[0]), sub(e[1], t[1])))
    return low + high


def real_dft(values):
    n = len(values)
    if n == 1:
        return [(values[0], None)]
    even, odd = real_dft(values[0::2]), real_dft(values[1::2])
    if n == 2:
        return [(even[0][0] + odd[0][0], None), (even[0][0] - odd[0][0], None)]
    out = [None] * (n // 2 + 1)
    for k in range(n // 4 + 1):
        t, e = turn(odd[k], k, n, -1), even[k]
        out[k] = (add(e[0], t[0]), add(e[1], t[1]))
        if n // 2 - k != k:
            out[n // 2 - k] = (sub(e[0], t[0]), sub(t[1], e[1]) if t[1] is not None else None if e[1] is None else -e[1])
    return out


def real_inverse(values):
    n = 2 * len(values) - 2
    if n == 2:
        return [values[0][0] + values[1][0], values[0][0] - values[1][0]]
    even, odd = [], []
    for k in range(n // 4 + 1):
        x, y = values[k], values[n // 2 - k]
        if n // 2 - k == k:
            even.append((2.0 * x[0], None))
            odd.append((-2.0 * x[1], None))
            continue
        even.append((x[0] + y[0], None if k == 0 else sub(x[1], y[1])))
        if k == 0:
            odd.append((x[0] - y[0], None))
        else:
            odd.append(turn((x[0] - y[0], add(x[1], y[1])), k, n, 1))
    even, odd = real_inverse(even), real_inverse(odd)
    return [v for both in zip(even, odd) for v in both]


def dot(a, b):
    return lax.dot_general(a, b, (((1,), (0,)), ((), ())), preferred_element_type=F32)


def split(x):
    high = x.astype(BF)
    return high, (x - high.astype(F32)).astype(BF)


def dot3(x, table):
    high, low = split(x)
    top = table[: x.shape[1]]
    return dot(jnp.concatenate([high, low, high], axis=1), jnp.concatenate([top, table], axis=0))


def iota(shape, dim):
    return lax.broadcasted_iota(jnp.int32, shape, dim)


def wrapped(p):
    return jnp.where(p >= 1.0 * N, p - 1.0 * N, p)


def block_swap(tiles, roll):
    block = iota((8, 128), 1) // 32
    turned = {(i, d): (roll(tiles[i], 32 * d) if d else tiles[i]) for i in range(4) for d in range(4)}
    out = []
    for q in range(4):
        acc = turned[(0, (0 - q) % 4)]
        for i in range(1, 4):
            acc = jnp.where(block == i, turned[(i, (i - q) % 4)], acc)
        out.append(acc)
    return out


def mixing(core, plane_of, bin_of, eff):
    col = iota((8, 128), 1)
    place = (col // 2) % 8
    slot = 2 * (place // 2) + jnp.where(core == 0, place % 2, 1 - place % 2)
    plane = jnp.zeros((8, 128), jnp.int32)
    for s in range(8):
        plane = jnp.where(slot == s, plane_of(s), plane)
    first_bin = jnp.zeros((8, 128), jnp.int32)
    weight = jnp.zeros((8, 128), F32)
    spread = jnp.concatenate([eff[b : b + 1] for b in range(4) for _ in range(2)], axis=0)
    for p in range(8):
        hit = plane == p
        first_bin = jnp.where(hit, bin_of(p), first_bin)
        weight = jnp.where(hit, spread[:, p : p + 1], weight)
    row = iota((8, 128), 0)
    weight = jnp.where((row // 2 >= first_bin) & (row % 2 == col % 2), weight, 0.0)
    mix = jnp.concatenate([jnp.where(col // 16 == 7 - t, weight, 0.0) for t in range(8)], axis=0)
    return jnp.concatenate(split(mix), axis=0)


def columns_body(dens, pos, table_of, twid, roll, emit):
    r, c = iota((32, 32), 0), iota((32, 32), 1)
    perm = jnp.where(c == 4 * (r % 8) + r // 8, 1.0, 0.0).astype(BF)
    dens_f = dot(perm, dens)
    dens_p = dens_f.astype(BF)
    left = jnp.concatenate([dens_p[:, 256 * a : 256 * (a + 1)] for a in range(8)], axis=0)
    lane, row = iota((32, 128), 1), iota((32, 128), 0)
    following = [dens_f[:, (256 * (a + 1)) % N : (256 * (a + 1)) % N + 1] for a in range(8)]
    cell = iota((256, 256), 0).astype(F32).astype(BF)
    zero = jnp.zeros((256, 256), BF)
    tiles = []
    for v in range(8):
        p = wrapped(pos[:, 256 * v : 256 * (v + 1)])
        group = jnp.floor(p * (1.0 / 256.0))
        local = p - 256.0 * group
        base = jnp.floor(local)
        here = (1.0 - (local - base)).astype(BF)
        there = (1.0 - (base + 1.0 - local)).astype(BF)
        table = jnp.where(cell == base.astype(BF), here, jnp.where(cell == (base + 1.0).astype(BF), there, zero))
        edge = jnp.where(base == 255.0, there.astype(F32), 0.0)
        parts = dot(left, table)
        acc, nxt = parts[0:32], jnp.broadcast_to(following[0], (32, 256))
        for a in range(1, 8):
            hit = group == 1.0 * a
            acc = jnp.where(hit, parts[32 * a : 32 * (a + 1)], acc)
            nxt = jnp.where(hit, following[a], nxt)
        acc = acc + edge * nxt
        tiles += [acc[:, :128], acc[:, 128:]]
    freq = real_dft(tiles)
    sign = jnp.where(lane % 2 == 0, 1.0, -1.0)
    nyquist = jnp.sum(freq[0][0] * sign, axis=1, keepdims=True)
    turned = []
    for m in range(16):
        re, im = freq[min(m, 16 - m)]
        co, si = twid[m : m + 1], twid[16 + m : 17 + m]
        if m == 0:
            im = jnp.zeros_like(re)
        elif im is None:
            re, im = re * co, -re * si
        elif m < 8:
            re, im = re * co + im * si, im * co - re * si
        else:
            re, im = re * co - im * si, -(im * co + re * si)
        turned.append(jnp.concatenate([re, im], axis=1))
    result = dot3(jnp.concatenate(turned, axis=0), table_of())
    for m in range(16):
        out = result[32 * m : 32 * m + 32]
        if m == 0:
            base = out[0:1, 0:1].astype(BF).astype(F32)
            out = jnp.where((lane == 0) & (row > 0), out - base, jnp.where(lane == 16, nyquist, out))
        emit(m, jnp.concatenate(block_swap([out[8 * i : 8 * i + 8] for i in range(4)], roll), axis=0).astype(BF))


def rows_body(got, pos, trans, ready, twid, twid_mixed, roll, emit):
    k1p, q = trans // 4, trans % 4
    turned = got.astype(F32).T
    marked = (iota((8, 512), 0) == 0) & (iota((8, 512), 1) % 8 == 0) & (trans == 0)
    base = jnp.where(marked, turned[0:8], 0.0)
    turned = jnp.concatenate([jnp.where(marked, 0.0, turned[0:8]), turned[8:]], axis=0)
    for step in (1, 2, 4):
        base = base + roll(base, step)
    left = jnp.concatenate([turned, roll(turned[0:32], 511), base, roll(base, 511)], axis=0).astype(BF)
    cell = iota((256, 256), 0).astype(F32).astype(BF)
    one, zero = jnp.ones((256, 256), BF), jnp.zeros((256, 256), BF)
    tiles = []
    for u in range(8):
        p = wrapped(pos[:, 256 * u : 256 * (u + 1)])
        group = jnp.floor(p * 0.25)
        local = p - 4.0 * group
        place = group - 8.0 * LEAD
        place = jnp.where(place < 0.0, place + 512.0, place)
        table = jnp.concatenate(
            [jnp.where(cell == place.astype(BF), one, zero), jnp.where(cell == (place - 256.0).astype(BF), one, zero)], axis=0
        )
        parts = dot(left, table)
        acc = total = None
        for s in range(5):
            weight = jnp.maximum(1.0 - jnp.abs(local - 1.0 * s), 0.0).astype(BF).astype(F32)
            acc = add(acc, weight * parts[32 * s : 32 * (s + 1)])
            if s < 4:
                total = add(total, weight)
        extra = total * parts[160:168] + weight * parts[168:176]
        acc = jnp.concatenate([acc[0:8] + extra, acc[8:32]], axis=0)
        tiles += [acc[:, :128], acc[:, 128:]]
    table2, table3, swap = ready()
    first = (iota((16, 128), 0) == 0) & (trans == 0)
    flat = [t[0:8] for t in tiles]
    total = flat[0]
    for t in flat[1:]:
        total = total + t
    mean = jnp.sum(total, axis=1, keepdims=True) * (1.0 / N)
    flat = dot(jnp.concatenate([t - mean for t in flat], axis=0).astype(BF), swap)
    values = []
    for t in tiles:
        re, im = t[0:16], t[16:32]
        values.append((jnp.where(first, im, re), jnp.where(first, 0.0, im)))
    freq = short_dft(values, -1)
    turned = []
    for m in range(16):
        re, im = freq[m]
        if m:
            co, si = twid[m : m + 1], twid[16 + m : 17 + m]
            re, im = re * co + im * si, im * co - re * si
        turned.append(jnp.concatenate([re, im], axis=1))
    spectrum = dot3(jnp.concatenate(turned, axis=0), table2)
    lane = iota((8, 128), 1)
    top = (iota((8, 128), 0) == 0) & (trans == 0)
    w2 = []
    for half in range(2):
        k2 = 256 * q + 16 * (iota((8, 128), 0) + 8 * half) + k1p
        w2.append((jnp.where(top, -HALF, k2) if half == 0 else k2).astype(F32))
    turned = []
    for m in range(16):
        k1 = m + 16 * lane
        w1 = jnp.where(k1 >= HALF, k1 - N, k1).astype(F32)
        square, double = w1 * w1, 2.0 * w1
        rows = [[], [], [], []]
        for half in range(2):
            base = 16 * m + 8 * half
            xr, xi = spectrum[base : base + 8, :128], spectrum[base : base + 8, 128:]
            other = w2[half] * w2[half]
            total = square + other
            inverse = 1.0 / (jnp.maximum(total, 1.0) if m == 0 else total)
            ka = (square - other) * inverse
            kb = double * w2[half] * inverse
            pr, pi = ka * xr, ka * xi
            if m == 0 or half == 0:
                edge = (w1 == -1.0 * HALF) if m == 0 else None
                if half == 0:
                    edge = top if edge is None else edge != top
                odd = jnp.where(edge, kb, 0.0)
                kb = jnp.where(edge, 0.0, kb)
                pr, pi = pr - odd * xi, pi + odd * xr
            for part, value in zip(rows, (pr, pi, kb * xr, kb * xi)):
                part.append(value)
        vr = jnp.concatenate(rows[0] + rows[2], axis=0)
        vi = jnp.concatenate(rows[1] + rows[3], axis=0)
        turned.append(jnp.concatenate([vr, vi], axis=1))
    result = dot3(jnp.concatenate(turned, axis=0), table3)
    back = []
    for m in range(16):
        re, im = result[32 * m : 32 * m + 32, :128], result[32 * m : 32 * m + 32, 128:]
        if m:
            co, si = twid_mixed[m : m + 1], twid_mixed[16 + m : 17 + m]
            re, im = re * co - im * si, im * co + re * si
        back.append((re, im))
    space = short_dft(back, 1)
    low_half = iota((64, 128), 1) < 64
    zero = jnp.zeros((8, 128), F32)
    stacked = []
    for n in range(16):
        re, im = space[n]
        real0 = jnp.concatenate([flat[8 * n : 8 * n + 8], zero], axis=0)
        r0, r1, i0, i1 = re[0:16], re[16:32], im[0:16], im[16:32]
        stacked.append(
            jnp.concatenate(
                [
                    jnp.where(first, real0, r0),
                    jnp.where(first, r0, i0),
                    jnp.where(first, 0.0, r1),
                    jnp.where(first, r1, i1),
                ],
                axis=0,
            )
        )
    for m in range(8):
        block = (TOP - m) % 8
        a, b = stacked[2 * block + 1], stacked[2 * block]
        top = jnp.where(low_half, a, roll(b, 64))
        bottom = jnp.where(low_half, roll(a, 64), b)
        emit(m, jnp.concatenate([top, bottom], axis=0).astype(BF).T)


def final_body(load, mix, table_of, twid, roll, emit):
    lane = iota((32, 128), 1)
    sign = jnp.where(lane % 2 == 0, 1.0, -1.0)
    lines = []
    for block in range(8):
        summed = dot(mix, load(block))
        summed = summed[0:64] + summed[64:128]
        for half in range(2):
            base = 32 * half
            line = jnp.concatenate(block_swap([summed[base + 8 * i : base + 8 * i + 8] for i in range(4)], roll), axis=0)
            if block == 0 and half == 0:
                nyquist = line[:, 16:17]
                line = jnp.where(lane == 0, 0.5 * line, line)
            lines.append(line)
    result = dot3(jnp.concatenate(lines, axis=0), table_of())
    values = []
    for m in range(16):
        re, im = result[32 * m : 32 * m + 32, :128], result[32 * m : 32 * m + 32, 128:]
        if m == 0:
            values.append((re + (nyquist * (1.0 / N)) * sign, None))
        else:
            co, si = twid[m : m + 1], twid[16 + m : 17 + m]
            values.append((re * co - im * si, im * co + re * si))
    terms = [values[0]]
    for m in range(1, 8):
        x, y = values[m], values[16 - m]
        terms.append((0.5 * (x[0] + y[0]), 0.5 * (x[1] - y[1])))
    terms.append((values[8][0], None))
    done = real_inverse(terms)
    for n in range(16):
        emit(n, done[n])


def rolled(x, shift):
    return pltpu.roll(x, shift, 1)


def start_copies(pairs, sems):
    copies = [pltpu.make_async_copy(src, dst, sems.at[n]) for n, (src, dst) in enumerate(pairs)]
    for copy in copies:
        copy.start()
    return copies


def columns_kernel(
    plane_hbm, bin_hbm, eff_hbm, dens_hbm, col_hbm, row_hbm, table_hbm, twid_hbm,
    out_ref, row_out, mix_out,
    plane_ref, bin_ref, eff_ref, dens_ref, col_ref, row_ref, table_ref, twid_ref, sems,
):
    pairs = [
        (plane_hbm, plane_ref), (dens_hbm, dens_ref), (col_hbm, col_ref), (twid_hbm, twid_ref),
        (table_hbm, table_ref), (row_hbm, row_ref), (bin_hbm, bin_ref), (eff_hbm, eff_ref),
    ]
    copies = start_copies(pairs, sems)
    for copy in copies:
        copy.wait()
    plane = plane_ref[lax.axis_index("los")]

    def emit(m, value):
        for q in range(4):
            place = 8 * ((4 * m + q - LEAD) % 64)
            out_ref[place : place + 8, :] = value[8 * q : 8 * q + 8]

    def table_of():
        row_out[...] = row_ref[pl.ds(plane, 1), :]
        mix_out[...] = mixing(lax.axis_index("los") % 2, lambda s: plane_ref[s], lambda p: bin_ref[p], eff_ref[...])
        return table_ref[...]

    columns_body(dens_ref[0], col_ref[pl.ds(plane, 1), :], table_of, twid_ref, rolled, emit)


def rows_kernel(got_ref, pos_ref, twid_ref, table2_ref, swap_ref, mixed_ref, table3_ref, same_ref, other_ref):
    north = lax.axis_index("los") % 2 == 1

    def emit(m, value):
        zero = jnp.concatenate([value[0:32], value[64:96]], axis=0)
        one = jnp.concatenate([value[32:64], value[96:128]], axis=0)
        same_ref[64 * m : 64 * m + 64, :] = jnp.where(north, one, zero)
        other_ref[64 * m : 64 * m + 64, :] = jnp.where(north, zero, one)

    def ready():
        return table2_ref[...], table3_ref[...], swap_ref[...]

    rows_body(got_ref[...], pos_ref[...], lax.axis_index("trans"), ready, twid_ref, mixed_ref, rolled, emit)


def final_kernel(got_ref, mix_ref, table_ref, twid_ref, out_ref, wide_ref):
    def emit(n, value):
        for g in range(4):
            jl, comp = g // 2, g % 2
            wide_ref[n, pl.ds(16 * comp + jl, 8, stride=2), :] = value[8 * g : 8 * g + 8]

    def table_of():
        return table_ref[...]

    final_body(
        lambda block: got_ref[pl.ds(128 * ((TOP - block) % 8), 128), :], mix_ref[...], table_of, twid_ref, rolled, emit
    )
    for n in range(16):
        for comp in range(2):
            for b in range(4):
                base = 16 * comp + 4 * b
                out_ref[comp, b, :, 128 * n : 128 * n + 128] = wide_ref[n, base : base + 4, :]


def call(kernel, shapes, near, far, scratch=()):
    vmem, hbm = (pl.BlockSpec(memory_space=m) for m in (pltpu.MemorySpace.VMEM, pltpu.MemorySpace.HBM))
    single = len(shapes) == 1
    return pl.pallas_call(
        kernel,
        out_shape=shapes[0] if single else shapes,
        in_specs=[vmem] * len(near) + [hbm] * len(far),
        out_specs=vmem if single else [vmem] * len(shapes),
        scratch_shapes=[pltpu.SMEM(a.shape, a.dtype) if a.ndim == 1 else pltpu.VMEM(a.shape, a.dtype) for a in far]
        + [pltpu.SemaphoreType.DMA((len(far),))] * bool(far)
        + list(scratch),
        compiler_params=pltpu.CompilerParams(vmem_limit_bytes=16 << 20),
    )(*near, *[pltpu.with_memory_space_constraint(jnp.asarray(a), pltpu.MemorySpace.HBM) for a in far])


def body(density, row_pos, col_pos, plane_of_slot, plane_bin, efficiency):
    first, second, back, final, swap, plain, mixed = tables()
    sent, row, mix = call(
        columns_kernel,
        [jax.ShapeDtypeStruct((512, 128), BF), jax.ShapeDtypeStruct((1, N), F32), jax.ShapeDtypeStruct((128, 128), BF)],
        [],
        [plane_of_slot, plane_bin, efficiency, density, col_pos, row_pos, pair(first), plain],
    )
    order = [[(n + LEAD) % 64 for n in range(64)]]
    got = lax.all_to_all(
        sent.reshape(64, 8, 128), "trans", split_axis=0, concat_axis=0, tiled=True, axis_index_groups=order
    )
    same, other = call(
        rows_kernel,
        [jax.ShapeDtypeStruct((512, 128), BF)] * 2,
        [got.reshape(512, 128), row, plain, pair(second), swap.astype(BF), mixed, pair(back)],
        [],
    )
    axes = ("trans", "los")
    other = lax.ppermute(other.reshape(256, 2, 128), axes, [(n, n ^ 1) for n in range(512)])
    sent = jnp.concatenate([same.reshape(256, 2, 128), other], axis=1)
    chips = [32 * ((TOP - m) % 8) + 28 - 4 * t + n for m in range(8) for t in range(8) for n in range(4)]
    order = [[2 * n + core for n in chips] for core in range(2)]
    got = lax.all_to_all(sent, axes, split_axis=0, concat_axis=0, tiled=True, axis_index_groups=order)
    return call(
        final_kernel,
        [jax.ShapeDtypeStruct((2, 4, 4, N), F32)],
        [got.reshape(1024, 128), mix, pair(final), plain],
        [],
        [pltpu.VMEM((16, 32, 128), F32)],
    )


def solution(mesh):
    placed = (P("los", "trans", None), P(), P(), P(), P(), P())
    return jax.shard_map(
        body,
        mesh=mesh,
        in_specs=placed,
        out_specs=P(None, None, ("trans", "los"), None),
        check_vma=False,
    )
```

```python
import math
import numpy as np
import jax
import jax.numpy as jnp
from jax import lax
from jax.sharding import PartitionSpec as P
from jax.experimental import pallas as pl
from jax.experimental.pallas import tpu as pltpu

BF = jnp.bfloat16
F32 = jnp.float32
N = 2048
HALF = 1024
LEAD = 63
TOP = 7


def pair(table):
    table = table.astype(np.float32)
    high = table.astype(BF)
    return np.concatenate([high, (table - high.astype(np.float32)).astype(BF)], axis=0)


def tables():
    n2 = np.arange(128)
    k2p = np.arange(64)
    angle = 2.0 * np.pi * np.outer(n2, k2p) / 128.0
    cos, sin = np.cos(angle).reshape(128, 4, 16), np.sin(angle).reshape(128, 4, 16)
    first = np.concatenate([np.stack([cos, -sin], 2), np.stack([sin, cos], 2)], 0).reshape(256, 128)
    angle = 2.0 * np.pi * np.outer(n2, n2) / 128.0
    cos, sin = np.cos(angle), np.sin(angle)
    second = np.block([[cos, -sin], [sin, cos]])
    order = np.arange(128).reshape(4, 4, 2, 2, 2)[::-1].transpose(4, 2, 0, 1, 3).reshape(-1)
    back = np.block([[cos[:, order], sin[:, order]], [-sin[:, order], cos[:, order]]]) / N
    angle = 2.0 * np.pi * np.outer(k2p, n2) / 128.0
    cos, sin = np.cos(angle).reshape(4, 16, 128), np.sin(angle).reshape(4, 16, 128)
    final = np.concatenate([np.stack([cos, -sin], 1), np.stack([sin, cos], 1)], 3).reshape(128, 256) * (2.0 / N)
    swap = np.zeros((128, 128))
    swap[order, np.arange(128)] = 1.0
    angle = 2.0 * np.pi * np.outer(np.arange(16), n2) / N
    plain = np.concatenate([np.cos(angle), np.sin(angle)], 0).astype(np.float32)
    mixed = np.concatenate([np.cos(angle[:, order]), np.sin(angle[:, order])], 0).astype(np.float32)
    return first, second, back, final, swap, plain, mixed


def add(a, b):
    return b if a is None else a if b is None else a + b


def sub(a, b):
    return a if b is None else -b if a is None else a - b


def turn(value, numer, denom, sign):
    re, im = value
    eighth = (8 * numer // denom) if (8 * numer) % denom == 0 else None
    if eighth == 0:
        return value
    if eighth == 2:
        if sign == 1:
            return (None if im is None else -im, re)
        return (im, -re)
    c, s = math.cos(2 * math.pi * numer / denom), sign * math.sin(2 * math.pi * numer / denom)
    if im is None:
        return (re * c, re * s)
    if re is None:
        return (im * -s, im * c)
    return (re * c - im * s, re * s + im * c)


def short_dft(values, sign):
    n = len(values)
    if n == 1:
        return values
    even = short_dft(values[0::2], sign)
    odd = short_dft(values[1::2], sign)
    low, high = [], []
    for k in range(n // 2):
        t = turn(odd[k], k, n, sign)
        e = even[k]
        low.append((add(e[0], t[0]), add(e[1], t[1])))
        high.append((sub(e[0], t[0]), sub(e[1], t[1])))
    return low + high


def real_dft(values):
    n = len(values)
    if n == 1:
        return [(values[0], None)]
    even, odd = real_dft(values[0::2]), real_dft(values[1::2])
    if n == 2:
        return [(even[0][0] + odd[0][0], None), (even[0][0] - odd[0][0], None)]
    out = [None] * (n // 2 + 1)
    for k in range(n // 4 + 1):
        t, e = turn(odd[k], k, n, -1), even[k]
        out[k] = (add(e[0], t[0]), add(e[1], t[1]))
        if n // 2 - k != k:
            out[n // 2 - k] = (sub(e[0], t[0]), sub(t[1], e[1]) if t[1] is not None else None if e[1] is None else -e[1])
    return out


def real_inverse(values):
    n = 2 * len(values) - 2
    if n == 2:
        return [values[0][0] + values[1][0], values[0][0] - values[1][0]]
    even, odd = [], []
    for k in range(n // 4 + 1):
        x, y = values[k], values[n // 2 - k]
        if n // 2 - k == k:
            even.append((2.0 * x[0], None))
            odd.append((-2.0 * x[1], None))
            continue
        even.append((x[0] + y[0], None if k == 0 else sub(x[1], y[1])))
        if k == 0:
            odd.append((x[0] - y[0], None))
        else:
            odd.append(turn((x[0] - y[0], add(x[1], y[1])), k, n, 1))
    even, odd = real_inverse(even), real_inverse(odd)
    return [v for both in zip(even, odd) for v in both]


def dot(a, b):
    return lax.dot_general(a, b, (((1,), (0,)), ((), ())), preferred_element_type=F32)


def split(x):
    high = x.astype(BF)
    return high, (x - high.astype(F32)).astype(BF)


def dot3(x, table):
    high, low = split(x)
    top = table[: x.shape[1]]
    return dot(jnp.concatenate([high, low, high], axis=1), jnp.concatenate([top, table], axis=0))


def iota(shape, dim):
    return lax.broadcasted_iota(jnp.int32, shape, dim)


def wrapped(p):
    return jnp.where(p >= 1.0 * N, p - 1.0 * N, p)


def block_swap(tiles, roll):
    block = iota((8, 128), 1) // 32
    turned = {(i, d): (roll(tiles[i], 32 * d) if d else tiles[i]) for i in range(4) for d in range(4)}
    out = []
    for q in range(4):
        acc = turned[(0, (0 - q) % 4)]
        for i in range(1, 4):
            acc = jnp.where(block == i, turned[(i, (i - q) % 4)], acc)
        out.append(acc)
    return out


def mixing(core, plane_of, bin_of, eff):
    col = iota((8, 128), 1)
    place = (col // 2) % 8
    slot = 2 * (place // 2) + jnp.where(core == 0, place % 2, 1 - place % 2)
    plane = jnp.zeros((8, 128), jnp.int32)
    for s in range(8):
        plane = jnp.where(slot == s, plane_of(s), plane)
    first_bin = jnp.zeros((8, 128), jnp.int32)
    weight = jnp.zeros((8, 128), F32)
    spread = jnp.concatenate([eff[b : b + 1] for b in range(4) for _ in range(2)], axis=0)
    for p in range(8):
        hit = plane == p
        first_bin = jnp.where(hit, bin_of(p), first_bin)
        weight = jnp.where(hit, spread[:, p : p + 1], weight)
    row = iota((8, 128), 0)
    weight = jnp.where((row // 2 >= first_bin) & (row % 2 == col % 2), weight, 0.0)
    mix = jnp.concatenate([jnp.where(col // 16 == 7 - t, weight, 0.0) for t in range(8)], axis=0)
    return jnp.concatenate(split(mix), axis=0)


def columns_body(dens, pos, table_of, twid, roll, emit):
    r, c = iota((32, 32), 0), iota((32, 32), 1)
    perm = jnp.where(c == 4 * (r % 8) + r // 8, 1.0, 0.0).astype(BF)
    dens_f = dot(perm, dens)
    dens_p = dens_f.astype(BF)
    left = jnp.concatenate([dens_p[:, 256 * a : 256 * (a + 1)] for a in range(8)], axis=0)
    lane, row = iota((32, 128), 1), iota((32, 128), 0)
    following = [dens_f[:, (256 * (a + 1)) % N : (256 * (a + 1)) % N + 1] for a in range(8)]
    cell = iota((256, 256), 0).astype(F32).astype(BF)
    zero = jnp.zeros((256, 256), BF)
    tiles = []
    for v in range(8):
        p = wrapped(pos[:, 256 * v : 256 * (v + 1)])
        group = jnp.floor(p * (1.0 / 256.0))
        local = p - 256.0 * group
        base = jnp.floor(local)
        here = (1.0 - (local - base)).astype(BF)
        there = (1.0 - (base + 1.0 - local)).astype(BF)
        table = jnp.where(cell == base.astype(BF), here, jnp.where(cell == (base + 1.0).astype(BF), there, zero))
        edge = jnp.where(base == 255.0, there.astype(F32), 0.0)
        parts = dot(left, table)
        acc, nxt = parts[0:32], jnp.broadcast_to(following[0], (32, 256))
        for a in range(1, 8):
            hit = group == 1.0 * a
            acc = jnp.where(hit, parts[32 * a : 32 * (a + 1)], acc)
            nxt = jnp.where(hit, following[a], nxt)
        acc = acc + edge * nxt
        tiles += [acc[:, :128], acc[:, 128:]]
    freq = real_dft(tiles)
    sign = jnp.where(lane % 2 == 0, 1.0, -1.0)
    nyquist = jnp.sum(freq[0][0] * sign, axis=1, keepdims=True)
    turned = []
    for m in range(16):
        re, im = freq[min(m, 16 - m)]
        co, si = twid[m : m + 1], twid[16 + m : 17 + m]
        if m == 0:
            im = jnp.zeros_like(re)
        elif im is None:
            re, im = re * co, -re * si
        elif m < 8:
            re, im = re * co + im * si, im * co - re * si
        else:
            re, im = re * co - im * si, -(im * co + re * si)
        turned.append(jnp.concatenate([re, im], axis=1))
    result = dot3(jnp.concatenate(turned, axis=0), table_of())
    for m in range(16):
        out = result[32 * m : 32 * m + 32]
        if m == 0:
            base = out[0:1, 0:1].astype(BF).astype(F32)
            out = jnp.where((lane == 0) & (row > 0), out - base, jnp.where(lane == 16, nyquist, out))
        emit(m, jnp.concatenate(block_swap([out[8 * i : 8 * i + 8] for i in range(4)], roll), axis=0).astype(BF))


def rows_body(got, pos, trans, ready, twid, twid_mixed, roll, emit):
    k1p, q = trans // 4, trans % 4
    turned = got.astype(F32).T
    marked = (iota((8, 512), 0) == 0) & (iota((8, 512), 1) % 8 == 0) & (trans == 0)
    base = jnp.where(marked, turned[0:8], 0.0)
    turned = jnp.concatenate([jnp.where(marked, 0.0, turned[0:8]), turned[8:]], axis=0)
    for step in (1, 2, 4):
        base = base + roll(base, step)
    left = jnp.concatenate([turned, roll(turned[0:32], 511), base, roll(base, 511)], axis=0).astype(BF)
    cell = iota((256, 256), 0).astype(F32).astype(BF)
    one, zero = jnp.ones((256, 256), BF), jnp.zeros((256, 256), BF)
    tiles = []
    for u in range(8):
        p = wrapped(pos[:, 256 * u : 256 * (u + 1)])
        group = jnp.floor(p * 0.25)
        local = p - 4.0 * group
        place = group - 8.0 * LEAD
        place = jnp.where(place < 0.0, place + 512.0, place)
        table = jnp.concatenate(
            [jnp.where(cell == place.astype(BF), one, zero), jnp.where(cell == (place - 256.0).astype(BF), one, zero)], axis=0
        )
        parts = dot(left, table)
        acc = total = None
        for s in range(5):
            weight = jnp.maximum(1.0 - jnp.abs(local - 1.0 * s), 0.0).astype(BF).astype(F32)
            acc = add(acc, weight * parts[32 * s : 32 * (s + 1)])
            if s < 4:
                total = add(total, weight)
        extra = total * parts[160:168] + weight * parts[168:176]
        acc = jnp.concatenate([acc[0:8] + extra, acc[8:32]], axis=0)
        tiles += [acc[:, :128], acc[:, 128:]]
    table2, table3, swap = ready()
    first = (iota((16, 128), 0) == 0) & (trans == 0)
    flat = [t[0:8] for t in tiles]
    total = flat[0]
    for t in flat[1:]:
        total = total + t
    mean = jnp.sum(total, axis=1, keepdims=True) * (1.0 / N)
    flat = dot(jnp.concatenate([t - mean for t in flat], axis=0).astype(BF), swap)
    values = []
    for t in tiles:
        re, im = t[0:16], t[16:32]
        values.append((jnp.where(first, im, re), jnp.where(first, 0.0, im)))
    freq = short_dft(values, -1)
    turned = []
    for m in range(16):
        re, im = freq[m]
        if m:
            co, si = twid[m : m + 1], twid[16 + m : 17 + m]
            re, im = re * co + im * si, im * co - re * si
        turned.append(jnp.concatenate([re, im], axis=1))
    spectrum = dot3(jnp.concatenate(turned, axis=0), table2)
    lane = iota((8, 128), 1)
    top = (iota((8, 128), 0) == 0) & (trans == 0)
    w2 = []
    for half in range(2):
        k2 = 256 * q + 16 * (iota((8, 128), 0) + 8 * half) + k1p
        w2.append((jnp.where(top, -HALF, k2) if half == 0 else k2).astype(F32))
    turned = []
    for m in range(16):
        k1 = m + 16 * lane
        w1 = jnp.where(k1 >= HALF, k1 - N, k1).astype(F32)
        square, double = w1 * w1, 2.0 * w1
        rows = [[], [], [], []]
        for half in range(2):
            base = 16 * m + 8 * half
            xr, xi = spectrum[base : base + 8, :128], spectrum[base : base + 8, 128:]
            other = w2[half] * w2[half]
            total = square + other
            inverse = 1.0 / (jnp.maximum(total, 1.0) if m == 0 else total)
            ka = (square - other) * inverse
            kb = double * w2[half] * inverse
            pr, pi = ka * xr, ka * xi
            if m == 0 or half == 0:
                edge = (w1 == -1.0 * HALF) if m == 0 else None
                if half == 0:
                    edge = top if edge is None else edge != top
                odd = jnp.where(edge, kb, 0.0)
                kb = jnp.where(edge, 0.0, kb)
                pr, pi = pr - odd * xi, pi + odd * xr
            for part, value in zip(rows, (pr, pi, kb * xr, kb * xi)):
                part.append(value)
        vr = jnp.concatenate(rows[0] + rows[2], axis=0)
        vi = jnp.concatenate(rows[1] + rows[3], axis=0)
        turned.append(jnp.concatenate([vr, vi], axis=1))
    result = dot3(jnp.concatenate(turned, axis=0), table3)
    back = []
    for m in range(16):
        re, im = result[32 * m : 32 * m + 32, :128], result[32 * m : 32 * m + 32, 128:]
        if m:
            co, si = twid_mixed[m : m + 1], twid_mixed[16 + m : 17 + m]
            re, im = re * co - im * si, im * co + re * si
        back.append((re, im))
    space = short_dft(back, 1)
    low_half = iota((64, 128), 1) < 64
    zero = jnp.zeros((8, 128), F32)
    stacked = []
    for n in range(16):
        re, im = space[n]
        real0 = jnp.concatenate([flat[8 * n : 8 * n + 8], zero], axis=0)
        r0, r1, i0, i1 = re[0:16], re[16:32], im[0:16], im[16:32]
        stacked.append(
            jnp.concatenate(
                [
                    jnp.where(first, real0, r0),
                    jnp.where(first, r0, i0),
                    jnp.where(first, 0.0, r1),
                    jnp.where(first, r1, i1),
                ],
                axis=0,
            )
        )
    for m in range(8):
        block = (TOP - m) % 8
        a, b = stacked[2 * block + 1], stacked[2 * block]
        top = jnp.where(low_half, a, roll(b, 64))
        bottom = jnp.where(low_half, roll(a, 64), b)
        emit(m, jnp.concatenate([top, bottom], axis=0).astype(BF).T)


def final_body(load, mix, table_of, twid, roll, emit):
    lane = iota((32, 128), 1)
    sign = jnp.where(lane % 2 == 0, 1.0, -1.0)
    lines = []
    for block in range(8):
        summed = dot(mix, load(block))
        summed = summed[0:64] + summed[64:128]
        for half in range(2):
            base = 32 * half
            line = jnp.concatenate(block_swap([summed[base + 8 * i : base + 8 * i + 8] for i in range(4)], roll), axis=0)
            if block == 0 and half == 0:
                nyquist = line[:, 16:17]
                line = jnp.where(lane == 0, 0.5 * line, line)
            lines.append(line)
    result = dot3(jnp.concatenate(lines, axis=0), table_of())
    values = []
    for m in range(16):
        re, im = result[32 * m : 32 * m + 32, :128], result[32 * m : 32 * m + 32, 128:]
        if m == 0:
            values.append((re + (nyquist * (1.0 / N)) * sign, None))
        else:
            co, si = twid[m : m + 1], twid[16 + m : 17 + m]
            values.append((re * co - im * si, im * co + re * si))
    terms = [values[0]]
    for m in range(1, 8):
        x, y = values[m], values[16 - m]
        terms.append((0.5 * (x[0] + y[0]), 0.5 * (x[1] - y[1])))
    terms.append((values[8][0], None))
    done = real_inverse(terms)
    for n in range(16):
        emit(n, done[n])


def rolled(x, shift):
    return pltpu.roll(x, shift, 1)


def start_copies(pairs, sems):
    copies = [pltpu.make_async_copy(src, dst, sems.at[n]) for n, (src, dst) in enumerate(pairs)]
    for copy in copies:
        copy.start()
    return copies


def columns_kernel(
    plane_hbm, bin_hbm, eff_hbm, dens_hbm, col_hbm, row_hbm, table_hbm, twid_hbm,
    out_ref, row_out, mix_out,
    plane_ref, bin_ref, eff_ref, dens_ref, col_ref, row_ref, table_ref, twid_ref, sems,
):
    pairs = [
        (plane_hbm, plane_ref), (dens_hbm, dens_ref), (col_hbm, col_ref), (twid_hbm, twid_ref),
        (table_hbm, table_ref), (row_hbm, row_ref), (bin_hbm, bin_ref), (eff_hbm, eff_ref),
    ]
    copies = start_copies(pairs, sems)
    for copy in copies:
        copy.wait()
    plane = plane_ref[lax.axis_index("los")]

    def emit(m, value):
        for q in range(4):
            place = 8 * ((4 * m + q - LEAD) % 64)
            out_ref[place : place + 8, :] = value[8 * q : 8 * q + 8]

    def table_of():
        row_out[...] = row_ref[pl.ds(plane, 1), :]
        mix_out[...] = mixing(lax.axis_index("los") % 2, lambda s: plane_ref[s], lambda p: bin_ref[p], eff_ref[...])
        return table_ref[...]

    columns_body(dens_ref[0], col_ref[pl.ds(plane, 1), :], table_of, twid_ref, rolled, emit)


def rows_kernel(got_ref, pos_ref, twid_ref, table2_ref, swap_ref, mixed_ref, table3_ref, same_ref, other_ref):
    north = lax.axis_index("los") % 2 == 1

    def emit(m, value):
        zero = jnp.concatenate([value[0:32], value[64:96]], axis=0)
        one = jnp.concatenate([value[32:64], value[96:128]], axis=0)
        same_ref[64 * m : 64 * m + 64, :] = jnp.where(north, one, zero)
        other_ref[64 * m : 64 * m + 64, :] = jnp.where(north, zero, one)

    def ready():
        return table2_ref[...], table3_ref[...], swap_ref[...]

    rows_body(got_ref[...], pos_ref[...], lax.axis_index("trans"), ready, twid_ref, mixed_ref, rolled, emit)


def final_kernel(got_ref, mix_ref, table_ref, twid_ref, out_ref, wide_ref):
    def emit(n, value):
        for g in range(4):
            jl, comp = g // 2, g % 2
            wide_ref[n, pl.ds(16 * comp + jl, 8, stride=2), :] = value[8 * g : 8 * g + 8]

    def table_of():
        return table_ref[...]

    final_body(
        lambda block: got_ref[pl.ds(128 * ((TOP - block) % 8), 128), :], mix_ref[...], table_of, twid_ref, rolled, emit
    )
    for n in range(16):
        for comp in range(2):
            for b in range(4):
                base = 16 * comp + 4 * b
                out_ref[comp, b, :, 128 * n : 128 * n + 128] = wide_ref[n, base : base + 4, :]


def call(kernel, shapes, near, far, scratch=()):
    vmem, hbm = (pl.BlockSpec(memory_space=m) for m in (pltpu.MemorySpace.VMEM, pltpu.MemorySpace.HBM))
    single = len(shapes) == 1
    return pl.pallas_call(
        kernel,
        out_shape=shapes[0] if single else shapes,
        in_specs=[vmem] * len(near) + [hbm] * len(far),
        out_specs=vmem if single else [vmem] * len(shapes),
        scratch_shapes=[pltpu.SMEM(a.shape, a.dtype) if a.ndim == 1 else pltpu.VMEM(a.shape, a.dtype) for a in far]
        + [pltpu.SemaphoreType.DMA((len(far),))] * bool(far)
        + list(scratch),
        compiler_params=pltpu.CompilerParams(vmem_limit_bytes=16 << 20),
    )(*near, *[pltpu.with_memory_space_constraint(jnp.asarray(a), pltpu.MemorySpace.HBM) for a in far])


def body(density, row_pos, col_pos, plane_of_slot, plane_bin, efficiency):
    first, second, back, final, swap, plain, mixed = tables()
    sent, row, mix = call(
        columns_kernel,
        [jax.ShapeDtypeStruct((512, 128), BF), jax.ShapeDtypeStruct((1, N), F32), jax.ShapeDtypeStruct((128, 128), BF)],
        [],
        [plane_of_slot, plane_bin, efficiency, density, col_pos, row_pos, pair(first), plain],
    )
    order = [[(n + LEAD) % 64 for n in range(64)]]
    got = lax.all_to_all(
        sent.reshape(64, 8, 128), "trans", split_axis=0, concat_axis=0, tiled=True, axis_index_groups=order
    )
    same, other = call(
        rows_kernel,
        [jax.ShapeDtypeStruct((512, 128), BF)] * 2,
        [got.reshape(512, 128), row, plain, pair(second), swap.astype(BF), mixed, pair(back)],
        [],
    )
    axes = ("trans", "los")
    other = lax.ppermute(other.reshape(256, 2, 128), axes, [(n, n ^ 1) for n in range(512)])
    sent = jnp.concatenate([same.reshape(256, 2, 128), other], axis=1)
    chips = [32 * ((TOP - m) % 8) + 28 - 4 * t + n for m in range(8) for t in range(8) for n in range(4)]
    order = [[2 * n + core for n in chips] for core in range(2)]
    got = lax.all_to_all(sent, axes, split_axis=0, concat_axis=0, tiled=True, axis_index_groups=order)
    return call(
        final_kernel,
        [jax.ShapeDtypeStruct((2, 4, 4, N), F32)],
        [got.reshape(1024, 128), mix, pair(final), plain],
        [],
        [pltpu.VMEM((16, 40, 128), F32)],
    )


def solution(mesh):
    placed = (P("los", "trans", None), P(), P(), P(), P(), P())
    return jax.shard_map(
        body,
        mesh=mesh,
        in_specs=placed,
        out_specs=P(None, None, ("trans", "los"), None),
        check_vma=False,
    )
```

```python
import math
import numpy as np
import jax
import jax.numpy as jnp
from jax import lax
from jax.sharding import PartitionSpec as P
from jax.experimental import pallas as pl
from jax.experimental.pallas import tpu as pltpu

BF = jnp.bfloat16
F32 = jnp.float32
N = 2048
HALF = 1024
LEAD = 63
TOP = 7


def pair(table):
    table = table.astype(np.float32)
    high = table.astype(BF)
    return np.concatenate([high, (table - high.astype(np.float32)).astype(BF)], axis=0)


def tables():
    n2 = np.arange(128)
    k2p = np.arange(64)
    angle = 2.0 * np.pi * np.outer(n2, k2p) / 128.0
    cos, sin = np.cos(angle).reshape(128, 4, 16), np.sin(angle).reshape(128, 4, 16)
    first = np.concatenate([np.stack([cos, -sin], 2), np.stack([sin, cos], 2)], 0).reshape(256, 128)
    angle = 2.0 * np.pi * np.outer(n2, n2) / 128.0
    cos, sin = np.cos(angle), np.sin(angle)
    second = np.block([[cos, -sin], [sin, cos]])
    order = np.arange(128).reshape(4, 4, 2, 2, 2)[::-1].transpose(4, 2, 0, 1, 3).reshape(-1)
    back = np.block([[cos[:, order], sin[:, order]], [-sin[:, order], cos[:, order]]]) / N
    angle = 2.0 * np.pi * np.outer(k2p, n2) / 128.0
    cos, sin = np.cos(angle).reshape(4, 16, 128), np.sin(angle).reshape(4, 16, 128)
    final = np.concatenate([np.stack([cos, -sin], 1), np.stack([sin, cos], 1)], 3).reshape(128, 256) * (2.0 / N)
    swap = np.zeros((128, 128))
    swap[order, np.arange(128)] = 1.0
    angle = 2.0 * np.pi * np.outer(np.arange(16), n2) / N
    plain = np.concatenate([np.cos(angle), np.sin(angle)], 0).astype(np.float32)
    mixed = np.concatenate([np.cos(angle[:, order]), np.sin(angle[:, order])], 0).astype(np.float32)
    return first, second, back, final, swap, plain, mixed


def add(a, b):
    return b if a is None else a if b is None else a + b


def sub(a, b):
    return a if b is None else -b if a is None else a - b


def turn(value, numer, denom, sign):
    re, im = value
    eighth = (8 * numer // denom) if (8 * numer) % denom == 0 else None
    if eighth == 0:
        return value
    if eighth == 2:
        if sign == 1:
            return (None if im is None else -im, re)
        return (im, -re)
    c, s = math.cos(2 * math.pi * numer / denom), sign * math.sin(2 * math.pi * numer / denom)
    if im is None:
        return (re * c, re * s)
    if re is None:
        return (im * -s, im * c)
    return (re * c - im * s, re * s + im * c)


def short_dft(values, sign):
    n = len(values)
    if n == 1:
        return values
    even = short_dft(values[0::2], sign)
    odd = short_dft(values[1::2], sign)
    low, high = [], []
    for k in range(n // 2):
        t = turn(odd[k], k, n, sign)
        e = even[k]
        low.append((add(e[0], t[0]), add(e[1], t[1])))
        high.append((sub(e[0], t[0]), sub(e[1], t[1])))
    return low + high


def real_dft(values):
    n = len(values)
    if n == 1:
        return [(values[0], None)]
    even, odd = real_dft(values[0::2]), real_dft(values[1::2])
    if n == 2:
        return [(even[0][0] + odd[0][0], None), (even[0][0] - odd[0][0], None)]
    out = [None] * (n // 2 + 1)
    for k in range(n // 4 + 1):
        t, e = turn(odd[k], k, n, -1), even[k]
        out[k] = (add(e[0], t[0]), add(e[1], t[1]))
        if n // 2 - k != k:
            out[n // 2 - k] = (sub(e[0], t[0]), sub(t[1], e[1]) if t[1] is not None else None if e[1] is None else -e[1])
    return out


def real_inverse(values):
    n = 2 * len(values) - 2
    if n == 2:
        return [values[0][0] + values[1][0], values[0][0] - values[1][0]]
    even, odd = [], []
    for k in range(n // 4 + 1):
        x, y = values[k], values[n // 2 - k]
        if n // 2 - k == k:
            even.append((2.0 * x[0], None))
            odd.append((-2.0 * x[1], None))
            continue
        even.append((x[0] + y[0], None if k == 0 else sub(x[1], y[1])))
        if k == 0:
            odd.append((x[0] - y[0], None))
        else:
            odd.append(turn((x[0] - y[0], add(x[1], y[1])), k, n, 1))
    even, odd = real_inverse(even), real_inverse(odd)
    return [v for both in zip(even, odd) for v in both]


def dot(a, b):
    return lax.dot_general(a, b, (((1,), (0,)), ((), ())), preferred_element_type=F32)


def split(x):
    high = x.astype(BF)
    return high, (x - high.astype(F32)).astype(BF)


def dot3(x, table):
    high, low = split(x)
    top = table[: x.shape[1]]
    return dot(jnp.concatenate([high, low, high], axis=1), jnp.concatenate([top, table], axis=0))


def iota(shape, dim):
    return lax.broadcasted_iota(jnp.int32, shape, dim)


def wrapped(p):
    return jnp.where(p >= 1.0 * N, p - 1.0 * N, p)


def block_swap(tiles, roll):
    block = iota((8, 128), 1) // 32
    turned = {(i, d): (roll(tiles[i], 32 * d) if d else tiles[i]) for i in range(4) for d in range(4)}
    out = []
    for q in range(4):
        acc = turned[(0, (0 - q) % 4)]
        for i in range(1, 4):
            acc = jnp.where(block == i, turned[(i, (i - q) % 4)], acc)
        out.append(acc)
    return out


def mixing(core, plane_of, bin_of, eff):
    col = iota((8, 128), 1)
    place = (col // 2) % 8
    slot = 2 * (place // 2) + jnp.where(core == 0, place % 2, 1 - place % 2)
    plane = jnp.zeros((8, 128), jnp.int32)
    for s in range(8):
        plane = jnp.where(slot == s, plane_of(s), plane)
    first_bin = jnp.zeros((8, 128), jnp.int32)
    weight = jnp.zeros((8, 128), F32)
    spread = jnp.concatenate([eff[b : b + 1] for b in range(4) for _ in range(2)], axis=0)
    for p in range(8):
        hit = plane == p
        first_bin = jnp.where(hit, bin_of(p), first_bin)
        weight = jnp.where(hit, spread[:, p : p + 1], weight)
    row = iota((8, 128), 0)
    weight = jnp.where((row // 2 >= first_bin) & (row % 2 == col % 2), weight, 0.0)
    mix = jnp.concatenate([jnp.where(col // 16 == 7 - t, weight, 0.0) for t in range(8)], axis=0)
    return jnp.concatenate(split(mix), axis=0)


def columns_body(dens, pos, table_of, twid, roll, emit):
    r, c = iota((32, 32), 0), iota((32, 32), 1)
    perm = jnp.where(c == 4 * (r % 8) + r // 8, 1.0, 0.0).astype(BF)
    dens_f = dot(perm, dens)
    dens_p = dens_f.astype(BF)
    left = jnp.concatenate([dens_p[:, 256 * a : 256 * (a + 1)] for a in range(8)], axis=0)
    lane, row = iota((32, 128), 1), iota((32, 128), 0)
    following = [dens_f[:, (256 * (a + 1)) % N : (256 * (a + 1)) % N + 1] for a in range(8)]
    cell = iota((256, 256), 0).astype(F32).astype(BF)
    zero = jnp.zeros((256, 256), BF)
    tiles = []
    for v in range(8):
        p = wrapped(pos[:, 256 * v : 256 * (v + 1)])
        group = jnp.floor(p * (1.0 / 256.0))
        local = p - 256.0 * group
        base = jnp.floor(local)
        here = (1.0 - (local - base)).astype(BF)
        there = (1.0 - (base + 1.0 - local)).astype(BF)
        table = jnp.where(cell == base.astype(BF), here, jnp.where(cell == (base + 1.0).astype(BF), there, zero))
        edge = jnp.where(base == 255.0, there.astype(F32), 0.0)
        parts = dot(left, table)
        acc, nxt = parts[0:32], jnp.broadcast_to(following[0], (32, 256))
        for a in range(1, 8):
            hit = group == 1.0 * a
            acc = jnp.where(hit, parts[32 * a : 32 * (a + 1)], acc)
            nxt = jnp.where(hit, following[a], nxt)
        acc = acc + edge * nxt
        tiles += [acc[:, :128], acc[:, 128:]]
    freq = real_dft(tiles)
    sign = jnp.where(lane % 2 == 0, 1.0, -1.0)
    nyquist = jnp.sum(freq[0][0] * sign, axis=1, keepdims=True)
    turned = []
    for m in range(16):
        re, im = freq[min(m, 16 - m)]
        co, si = twid[m : m + 1], twid[16 + m : 17 + m]
        if m == 0:
            im = jnp.zeros_like(re)
        elif im is None:
            re, im = re * co, -re * si
        elif m < 8:
            re, im = re * co + im * si, im * co - re * si
        else:
            re, im = re * co - im * si, -(im * co + re * si)
        turned.append(jnp.concatenate([re, im], axis=1))
    result = dot3(jnp.concatenate(turned, axis=0), table_of())
    for m in range(16):
        out = result[32 * m : 32 * m + 32]
        if m == 0:
            base = out[0:1, 0:1].astype(BF).astype(F32)
            out = jnp.where((lane == 0) & (row > 0), out - base, jnp.where(lane == 16, nyquist, out))
        emit(m, jnp.concatenate(block_swap([out[8 * i : 8 * i + 8] for i in range(4)], roll), axis=0).astype(BF))


def rows_body(got, pos, trans, ready, twid, twid_mixed, roll, emit):
    k1p, q = trans // 4, trans % 4
    turned = got.astype(F32).T
    marked = (iota((8, 512), 0) == 0) & (iota((8, 512), 1) % 8 == 0) & (trans == 0)
    base = jnp.where(marked, turned[0:8], 0.0)
    turned = jnp.concatenate([jnp.where(marked, 0.0, turned[0:8]), turned[8:]], axis=0)
    for step in (1, 2, 4):
        base = base + roll(base, step)
    left = jnp.concatenate([turned, roll(turned[0:32], 511), base, roll(base, 511)], axis=0).astype(BF)
    cell = iota((256, 256), 0).astype(F32).astype(BF)
    one, zero = jnp.ones((256, 256), BF), jnp.zeros((256, 256), BF)
    tiles = []
    for u in range(8):
        p = wrapped(pos[:, 256 * u : 256 * (u + 1)])
        group = jnp.floor(p * 0.25)
        local = p - 4.0 * group
        place = group - 8.0 * LEAD
        place = jnp.where(place < 0.0, place + 512.0, place)
        table = jnp.concatenate(
            [jnp.where(cell == place.astype(BF), one, zero), jnp.where(cell == (place - 256.0).astype(BF), one, zero)], axis=0
        )
        parts = dot(left, table)
        acc = total = None
        for s in range(5):
            weight = jnp.maximum(1.0 - jnp.abs(local - 1.0 * s), 0.0).astype(BF).astype(F32)
            acc = add(acc, weight * parts[32 * s : 32 * (s + 1)])
            if s < 4:
                total = add(total, weight)
        extra = total * parts[160:168] + weight * parts[168:176]
        acc = jnp.concatenate([acc[0:8] + extra, acc[8:32]], axis=0)
        tiles += [acc[:, :128], acc[:, 128:]]
    table2, table3, swap = ready()
    first = (iota((16, 128), 0) == 0) & (trans == 0)
    flat = [t[0:8] for t in tiles]
    total = flat[0]
    for t in flat[1:]:
        total = total + t
    mean = jnp.sum(total, axis=1, keepdims=True) * (1.0 / N)
    flat = dot(jnp.concatenate([t - mean for t in flat], axis=0).astype(BF), swap)
    values = []
    for t in tiles:
        re, im = t[0:16], t[16:32]
        values.append((jnp.where(first, im, re), jnp.where(first, 0.0, im)))
    freq = short_dft(values, -1)
    turned = []
    for m in range(16):
        re, im = freq[m]
        if m:
            co, si = twid[m : m + 1], twid[16 + m : 17 + m]
            re, im = re * co + im * si, im * co - re * si
        turned.append(jnp.concatenate([re, im], axis=1))
    spectrum = dot3(jnp.concatenate(turned, axis=0), table2)
    lane = iota((8, 128), 1)
    top = (iota((8, 128), 0) == 0) & (trans == 0)
    w2 = []
    for half in range(2):
        k2 = 256 * q + 16 * (iota((8, 128), 0) + 8 * half) + k1p
        w2.append((jnp.where(top, -HALF, k2) if half == 0 else k2).astype(F32))
    turned = []
    for m in range(16):
        k1 = m + 16 * lane
        w1 = jnp.where(k1 >= HALF, k1 - N, k1).astype(F32)
        square, double = w1 * w1, 2.0 * w1
        rows = [[], [], [], []]
        for half in range(2):
            base = 16 * m + 8 * half
            xr, xi = spectrum[base : base + 8, :128], spectrum[base : base + 8, 128:]
            other = w2[half] * w2[half]
            total = square + other
            inverse = 1.0 / (jnp.maximum(total, 1.0) if m == 0 else total)
            ka = (square - other) * inverse
            kb = double * w2[half] * inverse
            pr, pi = ka * xr, ka * xi
            if m == 0 or half == 0:
                edge = (w1 == -1.0 * HALF) if m == 0 else None
                if half == 0:
                    edge = top if edge is None else edge != top
                odd = jnp.where(edge, kb, 0.0)
                kb = jnp.where(edge, 0.0, kb)
                pr, pi = pr - odd * xi, pi + odd * xr
            for part, value in zip(rows, (pr, pi, kb * xr, kb * xi)):
                part.append(value)
        vr = jnp.concatenate(rows[0] + rows[2], axis=0)
        vi = jnp.concatenate(rows[1] + rows[3], axis=0)
        turned.append(jnp.concatenate([vr, vi], axis=1))
    result = dot3(jnp.concatenate(turned, axis=0), table3)
    back = []
    for m in range(16):
        re, im = result[32 * m : 32 * m + 32, :128], result[32 * m : 32 * m + 32, 128:]
        if m:
            co, si = twid_mixed[m : m + 1], twid_mixed[16 + m : 17 + m]
            re, im = re * co - im * si, im * co + re * si
        back.append((re, im))
    space = short_dft(back, 1)
    low_half = iota((64, 128), 1) < 64
    zero = jnp.zeros((8, 128), F32)
    stacked = []
    for n in range(16):
        re, im = space[n]
        real0 = jnp.concatenate([flat[8 * n : 8 * n + 8], zero], axis=0)
        r0, r1, i0, i1 = re[0:16], re[16:32], im[0:16], im[16:32]
        stacked.append(
            jnp.concatenate(
                [
                    jnp.where(first, real0, r0),
                    jnp.where(first, r0, i0),
                    jnp.where(first, 0.0, r1),
                    jnp.where(first, r1, i1),
                ],
                axis=0,
            )
        )
    for m in range(8):
        block = (TOP - m) % 8
        a, b = stacked[2 * block + 1], stacked[2 * block]
        top = jnp.where(low_half, a, roll(b, 64))
        bottom = jnp.where(low_half, roll(a, 64), b)
        emit(m, jnp.concatenate([top, bottom], axis=0).astype(BF).T)


def final_body(load, mix, table_of, twid, roll, emit):
    lane = iota((32, 128), 1)
    sign = jnp.where(lane % 2 == 0, 1.0, -1.0)
    lines = []
    for block in range(8):
        summed = dot(mix, load(block))
        summed = summed[0:64] + summed[64:128]
        for half in range(2):
            base = 32 * half
            line = jnp.concatenate(block_swap([summed[base + 8 * i : base + 8 * i + 8] for i in range(4)], roll), axis=0)
            if block == 0 and half == 0:
                nyquist = line[:, 16:17]
                line = jnp.where(lane == 0, 0.5 * line, line)
            lines.append(line)
    result = dot3(jnp.concatenate(lines, axis=0), table_of())
    values = []
    for m in range(16):
        re, im = result[32 * m : 32 * m + 32, :128], result[32 * m : 32 * m + 32, 128:]
        if m == 0:
            values.append((re + (nyquist * (1.0 / N)) * sign, None))
        else:
            co, si = twid[m : m + 1], twid[16 + m : 17 + m]
            values.append((re * co - im * si, im * co + re * si))
    terms = [values[0]]
    for m in range(1, 8):
        x, y = values[m], values[16 - m]
        terms.append((0.5 * (x[0] + y[0]), 0.5 * (x[1] - y[1])))
    terms.append((values[8][0], None))
    done = real_inverse(terms)
    for n in range(16):
        emit(n, done[n])


def rolled(x, shift):
    return pltpu.roll(x, shift, 1)


def start_copies(pairs, sems):
    copies = [pltpu.make_async_copy(src, dst, sems.at[n]) for n, (src, dst) in enumerate(pairs)]
    for copy in copies:
        copy.start()
    return copies


def columns_kernel(
    plane_hbm, bin_hbm, eff_hbm, dens_hbm, col_hbm, row_hbm, table_hbm, twid_hbm,
    out_ref, row_out, mix_out,
    plane_ref, bin_ref, eff_ref, dens_ref, col_ref, row_ref, table_ref, twid_ref, sems,
):
    pairs = [
        (plane_hbm, plane_ref), (dens_hbm, dens_ref), (col_hbm, col_ref), (twid_hbm, twid_ref),
        (table_hbm, table_ref), (row_hbm, row_ref), (bin_hbm, bin_ref), (eff_hbm, eff_ref),
    ]
    copies = start_copies(pairs, sems)
    for copy in copies[:4]:
        copy.wait()
    plane = plane_ref[lax.axis_index("los")]

    def emit(m, value):
        for q in range(4):
            place = 8 * ((4 * m + q - LEAD) % 64)
            out_ref[place : place + 8, :] = value[8 * q : 8 * q + 8]

    def table_of():
        for copy in copies[4:]:
            copy.wait()
        row_out[...] = row_ref[pl.ds(plane, 1), :]
        mix_out[...] = mixing(lax.axis_index("los") % 2, lambda s: plane_ref[s], lambda p: bin_ref[p], eff_ref[...])
        return table_ref[...]

    columns_body(dens_ref[0], col_ref[pl.ds(plane, 1), :], table_of, twid_ref, rolled, emit)


def rows_kernel(got_ref, pos_ref, twid_ref, table2_ref, swap_ref, mixed_ref, table3_ref, same_ref, other_ref):
    north = lax.axis_index("los") % 2 == 1

    def emit(m, value):
        zero = jnp.concatenate([value[0:32], value[64:96]], axis=0)
        one = jnp.concatenate([value[32:64], value[96:128]], axis=0)
        same_ref[64 * m : 64 * m + 64, :] = jnp.where(north, one, zero)
        other_ref[64 * m : 64 * m + 64, :] = jnp.where(north, zero, one)

    def ready():
        return table2_ref[...], table3_ref[...], swap_ref[...]

    rows_body(got_ref[...], pos_ref[...], lax.axis_index("trans"), ready, twid_ref, mixed_ref, rolled, emit)


def final_kernel(got_ref, mix_ref, table_ref, twid_ref, out_ref, wide_ref):
    def emit(n, value):
        for g in range(4):
            jl, comp = g // 2, g % 2
            wide_ref[n, pl.ds(16 * comp + jl, 8, stride=2), :] = value[8 * g : 8 * g + 8]

    def table_of():
        return table_ref[...]

    final_body(
        lambda block: got_ref[pl.ds(128 * ((TOP - block) % 8), 128), :], mix_ref[...], table_of, twid_ref, rolled, emit
    )
    for n in range(16):
        for comp in range(2):
            for b in range(4):
                base = 16 * comp + 4 * b
                out_ref[comp, b, :, 128 * n : 128 * n + 128] = wide_ref[n, base : base + 4, :]


def call(kernel, shapes, near, far, scratch=()):
    vmem, hbm = (pl.BlockSpec(memory_space=m) for m in (pltpu.MemorySpace.VMEM, pltpu.MemorySpace.HBM))
    single = len(shapes) == 1
    return pl.pallas_call(
        kernel,
        out_shape=shapes[0] if single else shapes,
        in_specs=[vmem] * len(near) + [hbm] * len(far),
        out_specs=vmem if single else [vmem] * len(shapes),
        scratch_shapes=[pltpu.SMEM(a.shape, a.dtype) if a.ndim == 1 else pltpu.VMEM(a.shape, a.dtype) for a in far]
        + [pltpu.SemaphoreType.DMA((len(far),))] * bool(far)
        + list(scratch),
        compiler_params=pltpu.CompilerParams(vmem_limit_bytes=16 << 20),
    )(*near, *[pltpu.with_memory_space_constraint(jnp.asarray(a), pltpu.MemorySpace.HBM) for a in far])


def body(density, row_pos, col_pos, plane_of_slot, plane_bin, efficiency):
    first, second, back, final, swap, plain, mixed = tables()
    sent, row, mix = call(
        columns_kernel,
        [jax.ShapeDtypeStruct((512, 128), BF), jax.ShapeDtypeStruct((1, N), F32), jax.ShapeDtypeStruct((128, 128), BF)],
        [],
        [plane_of_slot, plane_bin, efficiency, density, col_pos, row_pos, pair(first), plain],
    )
    order = [[(n + LEAD) % 64 for n in range(64)]]
    got = lax.all_to_all(
        sent.reshape(64, 8, 128), "trans", split_axis=0, concat_axis=0, tiled=True, axis_index_groups=order
    )
    same, other = call(
        rows_kernel,
        [jax.ShapeDtypeStruct((512, 128), BF)] * 2,
        [got.reshape(512, 128), row, plain, pair(second), swap.astype(BF), mixed, pair(back)],
        [],
    )
    axes = ("trans", "los")
    other = lax.ppermute(other.reshape(256, 2, 128), axes, [(n, n ^ 1) for n in range(512)])
    sent = jnp.concatenate([same.reshape(256, 2, 128), other], axis=1)
    chips = [32 * ((TOP - m) % 8) + 28 - 4 * t + n for m in range(8) for t in range(8) for n in range(4)]
    order = [[2 * n + core for n in chips] for core in range(2)]
    got = lax.all_to_all(sent, axes, split_axis=0, concat_axis=0, tiled=True, axis_index_groups=order)
    return call(
        final_kernel,
        [jax.ShapeDtypeStruct((2, 4, 4, N), F32)],
        [got.reshape(1024, 128), mix, pair(final), plain],
        [],
        [pltpu.VMEM((16, 40, 128), F32)],
    )


def solution(mesh):
    placed = (P("los", "trans", None), P(), P(), P(), P(), P())
    return jax.shard_map(
        body,
        mesh=mesh,
        in_specs=placed,
        out_specs=P(None, None, ("trans", "los"), None),
        check_vma=False,
    )
```
